128 devices in a mesh: act: 4 (over y), virt: 32 (over x, z, core).
Axes of the slice: x: 4, y: 4, z: 4, core: 2. Of those that a mesh axis runs over, the one named last changes fastest.
Arguments:
- amplitudes: bfloat16 [400, 640, 640], P('act', 'virt'), may hold values from -6 to 6
- virtual_fock_block: bfloat16 [640, 640], replicated, may hold values from -1 to 3.1, as said below
- metric: bfloat16 [400, 400], replicated, may hold values from -3.5 to 3.5, as said below
- active_block: bfloat16 [400, 400], replicated, may hold values from -0.3125 to 0.3125
Outputs:
- residual_vec: bfloat16 [400, 640, 640], P('act', 'virt')
- rayleigh: float32 [], replicated
- res_norm: float32 [], replicated
The draws below stay inside these ranges and needn't reach their ends.
Inputs may be any that keep to these rules, and one draw needn't show every extreme that they name: `virtual_fock_block`: symmetric. `metric`: symmetric positive definite.
All inputs are finite; a program needn't handle non-finite values.
Results may differ from the reference program's by a relative error of at most 0.0099.
Values may be sent and summed in bfloat16 or wider, within the bound.
A program may use at most 128 MiB of HBM per device.

```python
import jax
import jax.numpy as jnp
from jax import lax

NV = 640
TU = 400


def draw_virtual_fock_block(key, part):
    leading_key, second_key = jax.random.split(jax.random.fold_in(key, 11))
    energies = jax.random.uniform(leading_key, (NV,), jnp.float32, 0.5, 3.0)
    coupling = jax.random.uniform(second_key, (NV, NV), jnp.float32, -1.0, 1.0) * 1.7
    coupling = (coupling + coupling.T) * (0.35 / math_sqrt(NV))
    coupling = coupling * (1.0 - jnp.eye(NV, dtype=jnp.float32))
    return (jnp.diag(energies) + coupling).astype(jnp.bfloat16)


def math_sqrt(value):
    return float(value) ** 0.5


def draw_metric(key, part):
    leading_key = jax.random.fold_in(jax.random.fold_in(key, 23), 0)
    factor = jax.random.uniform(leading_key, (TU, TU), jnp.float32, -1.7, 1.7)
    product = jnp.dot(factor, factor.T, precision=lax.Precision.HIGHEST) / TU
    return (0.5 * jnp.eye(TU, dtype=jnp.float32) + product).astype(jnp.bfloat16)


def level_of(own_key, extent, pieces, least, top_value):
    level, own = 1.0, jax.random.fold_in(own_key, 6)
    for axis_at, shards_of in pieces:
        heights = jnp.exp(jax.random.uniform(jax.random.fold_in(own, axis_at), (shards_of,), jnp.float32, least / len(pieces), top_value / len(pieces)))
        level = level * jnp.repeat(heights, extent[axis_at] // shards_of).reshape([-1 if axis == axis_at else 1 for axis in range(len(extent))])
    return level


def noise(key, shape, scale, most, shards=(), held_as=jnp.bfloat16):
    drawn = jax.random.normal(key, shape, jnp.float32) * scale
    if len(shards) > 0:
        drawn = level_of(key, shape, shards, -0.22, 0.18) * drawn
    return jnp.clip(drawn, min=-most, max=most).astype(held_as)


def setup_inputs(seed: int = 0) -> dict:
    keys = jax.random.split(jax.random.key(seed), 5)
    amplitudes = noise(keys[0], (TU, NV, NV), 1.0, 6.0, ((0, 4), (1, 32)))
    virtual_fock_block = draw_virtual_fock_block(jax.random.fold_in(keys[4], 71), 0)
    metric = draw_metric(jax.random.fold_in(keys[4], 71), 0)
    active_block = noise(keys[3], (TU, TU), TU ** -0.5, 0.3125)
    return dict(amplitudes=amplitudes, virtual_fock_block=virtual_fock_block, metric=metric, active_block=active_block)


def reference(amplitudes, virtual_fock_block, metric, active_block):
    broadened_fock = virtual_fock_block.astype(jnp.float32)
    block_of_rows = 32
    blocks_count = NV // block_of_rows
    indices = jnp.arange(blocks_count, dtype=jnp.int32)

    def metric_rows(index):
        start = (index * block_of_rows).astype(jnp.int32)
        trial_rows = lax.dynamic_slice_in_dim(amplitudes, start, block_of_rows, 1)
        flat_trial = trial_rows.reshape(TU, block_of_rows * NV)
        weighted_rows = jnp.dot(metric, flat_trial, preferred_element_type=jnp.float32)
        return weighted_rows.astype(jnp.bfloat16).reshape(TU, block_of_rows, NV)

    half_blocks = lax.map(metric_rows, indices)
    weighted_half = jnp.moveaxis(half_blocks, 0, 1).reshape(TU, NV, NV)

    def left_group(group_rows):
        return jnp.einsum("ac,tcb->tab", broadened_fock, group_rows.astype(jnp.float32)).astype(jnp.bfloat16)

    left_portion = lax.map(left_group, weighted_half.reshape(TU // 4, 4, NV, NV)).reshape(TU, NV, NV)

    def project(index):
        start = (index * block_of_rows).astype(jnp.int32)
        trial_rows = lax.dynamic_slice_in_dim(amplitudes, start, block_of_rows, 1)
        halved_rows = lax.dynamic_slice_in_dim(weighted_half, start, block_of_rows, 1)
        left_rows = lax.dynamic_slice_in_dim(left_portion, start, block_of_rows, 1)
        flat_trial = trial_rows.reshape(TU, block_of_rows * NV)
        rightside_rows = jnp.einsum("wuv,vq->wuq", halved_rows.astype(jnp.float32), broadened_fock)
        sigma_rows = left_rows.astype(jnp.float32).reshape(TU, block_of_rows * NV) + rightside_rows.reshape(TU, block_of_rows * NV) + jnp.dot(active_block, flat_trial, preferred_element_type=jnp.float32)
        weighted_rows = jnp.dot(metric, flat_trial, preferred_element_type=jnp.float32)
        return sigma_rows, weighted_rows, flat_trial.astype(jnp.float32)

    def intersect(index):
        sigma_rows, weighted_rows, trial_wide = project(index)
        return jnp.sum(trial_wide * sigma_rows), jnp.sum(trial_wide * weighted_rows)

    numer_parts, denom_parts = lax.map(intersect, indices)
    numerator = jnp.sum(numer_parts)
    denominator = jnp.sum(denom_parts)
    rayleigh = numerator / denominator

    def finish(index):
        sigma_rows, weighted_rows, trial_wide = project(index)
        resid = sigma_rows - rayleigh * weighted_rows
        return resid.astype(jnp.bfloat16).reshape(TU, block_of_rows, NV), jnp.sum(resid * resid)

    resid_blocks, square_parts = lax.map(finish, indices)
    residual_vec = jnp.moveaxis(resid_blocks, 0, 1).reshape(TU, NV, NV)
    res_norm = jnp.sum(square_parts) / denominator
    return residual_vec, rayleigh, res_norm
```

```python
import functools

import jax
import jax.numpy as jnp
from jax import lax
from jax.experimental import pallas as pl
from jax.experimental.pallas import tpu as pltpu
from jax.sharding import PartitionSpec as P

MESH = pl.DeviceIdType.MESH
LANES = 128
F32, BF16 = jnp.float32, jnp.bfloat16


def round_up(value, unit):
    return -(-value // unit) * unit


def one_hot(shape, place, axis, every, gap):
    index = lax.broadcasted_iota(jnp.int32, shape, axis)
    other = lax.broadcasted_iota(jnp.int32, shape, 1 - axis)
    return jnp.where(index + gap * (index // every) + place == other, 1.0, 0.0).astype(BF16)


def sigma_kernel(groups, peers, x_ref, fock_ref, metric_ref, active_ref, out_ref, stats_ref,
                 trial, fock, metric, active, spread, mats, gathered, surplus, leaving, local, coming,
                 trial_wide, image_wide, image, held, made, back, sigma, row_sums, sum_slots,
                 loaded, small_loaded, row_sent, row_landed, field_sent, field_landed,
                 sent, landed, spare_sent, spare_landed,
                 back_sent, back_landed, back_spare_sent, back_spare_landed,
                 stored, sum_sent, sum_landed):
    group, me = lax.axis_index("act"), lax.axis_index("virt")
    chunks, pairs, tall = trial.shape[0], trial.shape[1], trial.shape[2]
    rows = x_ref.shape[1]
    width = x_ref.shape[2]
    high = gathered.shape[4]
    part = rows // groups
    share, spares = pairs // peers, pairs % peers
    stride = peers // spares
    right, left = lax.rem(group + 1, groups), lax.rem(group + groups - 1, groups)
    opposite = lax.rem(group + 2, groups)
    real = pl.ds(0, rows)
    real_pairs = pl.ds(0, pairs)

    def load(c):
        return pltpu.make_async_copy(
            x_ref.at[:, :, pl.ds(pl.multiple_of(c * LANES, LANES), LANES)], trial.at[c, :, real], loaded.at[c])

    smalls = [pltpu.make_async_copy(source, target, small_loaded.at[i]) for i, (source, target) in enumerate(
        ((metric_ref, metric), (active_ref, active), (fock_ref, fock)))]
    for c in range(chunks):
        load(c).start()
    for copy in smalls:
        copy.start()

    extra = pl.ds(rows, tall - rows)
    zero_rows = tall - rows

    def clear(c, carry):
        held[c, :, :, extra] = jnp.zeros(held.shape[1:3] + (zero_rows, LANES), BF16)
        back[c, :, extra] = jnp.zeros((pairs, zero_rows, LANES), BF16)
        trial[c, :, extra] = jnp.zeros((pairs, zero_rows, LANES), BF16)
        for q in range(zero_rows):
            sigma[c, pl.ds(rows + q, high, stride=tall)] = jnp.zeros((high, LANES), F32)
        gathered[c, :, :, :, pl.ds(pairs, high - pairs)] = jnp.zeros(
            gathered.shape[1:4] + (high - pairs, LANES), BF16)
        return carry

    lax.fori_loop(0, chunks, clear, 0)
    trial_wide[pl.ds(pairs * tall, (high - pairs) * tall)] = jnp.zeros(((high - pairs) * tall, LANES), F32)
    for q in range(zero_rows):
        image_wide[pl.ds(rows + q, high, stride=tall)] = jnp.zeros((high, LANES), F32)

    barrier = pltpu.get_barrier_semaphore()

    def greet(step, carry):
        pl.semaphore_signal(barrier, inc=1, device_id=(group, lax.rem(me + step, peers)), device_id_type=MESH)
        return carry

    lax.fori_loop(1, peers, greet, 0)
    for step in range(1, groups):
        pl.semaphore_signal(barrier, inc=1, device_id=(lax.rem(group + step, groups), me), device_id_type=MESH)
    pl.semaphore_wait(barrier, peers + groups - 2)

    def row_copy(c, which, source, kind, owner, target):
        return pltpu.make_async_remote_copy(
            src_ref=source.at[:, real_pairs], dst_ref=gathered.at[c, kind, owner, :, real_pairs],
            send_sem=row_sent.at[c, which], recv_sem=row_landed.at[c, kind, owner],
            device_id=(target, me), device_id_type=MESH)

    def row_sends(c):
        return (
            row_copy(c, 0, surplus.at[c, 0], 0, group, right),
            row_copy(c, 1, surplus.at[c, 1], 1, group, left),
            row_copy(c, 2, gathered.at[c, 0, group], 1, group, right),
            row_copy(c, 3, gathered.at[c, 1, group], 0, group, left))

    def row_forwards(c):
        return (
            row_copy(c, 4, gathered.at[c, 0, left], 1, left, right),
            row_copy(c, 5, gathered.at[c, 1, right], 0, right, left))

    def row_arrival(c, kind, owner):
        return row_copy(c, 0, surplus.at[c, 0], kind, owner, right)

    def field_copy(c, kind):
        return pltpu.make_async_remote_copy(
            src_ref=leaving.at[c, kind, :, :, real_pairs], dst_ref=coming.at[c, kind, :, :, real_pairs],
            send_sem=field_sent.at[c, kind], recv_sem=field_landed.at[c, kind],
            device_id=((left, right)[kind], me), device_id_type=MESH)

    def spare_place(c):
        return lax.rem(2 * c + c // 4, stride)

    def peer_at(step):
        return lax.rem(me + step, peers)

    def forward(c, peer):
        return pltpu.make_async_remote_copy(
            src_ref=image.at[c, pl.ds(peer * share, share), real],
            dst_ref=held.at[c, pl.ds(0, share), me, real],
            send_sem=sent.at[c, peer], recv_sem=landed.at[c, me],
            device_id=(group, peer), device_id_type=MESH)

    def arrival(c, peer):
        return pltpu.make_async_remote_copy(
            src_ref=image.at[c, pl.ds(peer * share, share), real],
            dst_ref=held.at[c, pl.ds(0, share), peer, real],
            send_sem=sent.at[c, peer], recv_sem=landed.at[c, peer],
            device_id=(group, peer), device_id_type=MESH)

    def spare_forward(c, j, peer):
        return pltpu.make_async_remote_copy(
            src_ref=image.at[c, share * peers + j, real], dst_ref=held.at[c, share, me, real],
            send_sem=spare_sent.at[c, j], recv_sem=spare_landed.at[c, me],
            device_id=(group, peer), device_id_type=MESH)

    def spare_arrival(c, peer):
        return pltpu.make_async_remote_copy(
            src_ref=image.at[c, share * peers, real], dst_ref=held.at[c, share, peer, real],
            send_sem=spare_sent.at[c, 0], recv_sem=spare_landed.at[c, peer],
            device_id=(group, peer), device_id_type=MESH)

    def backward(c, peer):
        return pltpu.make_async_remote_copy(
            src_ref=made.at[c, pl.ds(0, share), peer, real],
            dst_ref=back.at[c, pl.ds(me * share, share), real],
            send_sem=back_sent.at[c, peer], recv_sem=back_landed.at[c, me],
            device_id=(group, peer), device_id_type=MESH)

    def back_arrival(c, peer):
        return pltpu.make_async_remote_copy(
            src_ref=made.at[c, pl.ds(0, share), peer, real],
            dst_ref=back.at[c, pl.ds(peer * share, share), real],
            send_sem=back_sent.at[c, peer], recv_sem=back_landed.at[c, peer],
            device_id=(group, peer), device_id_type=MESH)

    def spare_backward(c, peer):
        return pltpu.make_async_remote_copy(
            src_ref=made.at[c, share, peer, real],
            dst_ref=back.at[c, share * peers + me // stride, real],
            send_sem=back_spare_sent.at[c, peer], recv_sem=back_spare_landed.at[c, me // stride],
            device_id=(group, peer), device_id_type=MESH)

    def spare_back_arrival(c, j, peer):
        return pltpu.make_async_remote_copy(
            src_ref=made.at[c, share, peer, real], dst_ref=back.at[c, share * peers + j, real],
            send_sem=back_spare_sent.at[c, peer], recv_sem=back_spare_landed.at[c, j],
            device_id=(group, peer), device_id_type=MESH)

    def owns_spare(c):
        return lax.rem(me, stride) == spare_place(c)

    def send_rows(c):
        load(c).wait()

        def widen(b, carry):
            trial_wide[pl.ds(pl.multiple_of(b * 10 * tall, 8), 10 * tall)] = trial[
                c, pl.ds(b * 10, 10)].astype(F32).reshape(10 * tall, LANES)
            return carry

        lax.fori_loop(0, pairs // 10, widen, 0)
        for p in range(groups):
            first = lax.rem(group + p, groups) * part
            for j in range(part):
                turned = trial_wide[pl.ds(first + j, high, stride=tall)].astype(BF16)
                if p == 0:
                    gathered[c, 0, group, j] = turned
                elif p == groups - 1:
                    gathered[c, 1, group, j] = turned
                else:
                    surplus[c, p - 1, j] = turned
        for copy in row_sends(c):
            copy.start()

    def prepare():
        for copy in smalls:
            copy.wait()
        count = groups * pairs
        spread_pairs = one_hot((count, groups * high), 0, 0, pairs, high - pairs)
        for which, matrix in enumerate((metric, active)):
            wide = jnp.dot(matrix[...], spread_pairs, preferred_element_type=F32).astype(BF16)
            for kind in range(2):
                at = lax.broadcasted_iota(jnp.int32, (2 * high, count), 0)
                column = lax.broadcasted_iota(jnp.int32, (2 * high, count), 1)
                other = left if kind == 0 else right
                wanted = jnp.where(at < high, at + group * pairs, at - high + other * pairs)
                kept = jnp.where(at < high, at, at - high) < pairs
                choose = jnp.where((wanted == column) & kept, 1.0, 0.0).astype(BF16)
                mats[kind, pl.ds(2 * high * which, 2 * high)] = jnp.dot(
                    choose, wide, preferred_element_type=F32).astype(BF16)
        across = one_hot((width, peers * tall), 0, 0, rows, tall - rows)
        down = one_hot((peers * tall, width), 0, 1, rows, tall - rows)
        half = jnp.dot(fock[...], across, preferred_element_type=F32).astype(BF16)
        spread[...] = jnp.dot(down, half, preferred_element_type=F32).astype(BF16)

    def shift_of():
        at = lax.broadcasted_iota(jnp.int32, fock.shape, 0)
        column = lax.broadcasted_iota(jnp.int32, fock.shape, 1)
        diagonal = jnp.where(at == column, fock[...].astype(F32), 0.0)
        return (2.0 / width) * jnp.sum(jnp.sum(diagonal, axis=0, keepdims=True), axis=1, keepdims=True)

    def pass_rows(c):
        row_arrival(c, 0, left).wait_recv()
        row_arrival(c, 1, right).wait_recv()
        for copy in row_forwards(c):
            copy.start()

    def mix(c):
        shift = row_sums[0, 0:1, 0:1]
        row_arrival(c, 0, right).wait_recv()
        row_arrival(c, 1, left).wait_recv()
        row_arrival(c, 0, opposite).wait_recv()
        row_arrival(c, 1, opposite).wait_recv()
        for kind in range(2):
            block = jnp.concatenate(
                [gathered[c, kind, :, j].reshape(groups * high, LANES) for j in range(part)], axis=1)
            both = jnp.dot(mats[kind], block, preferred_element_type=F32)
            weighted = both[:2 * high]
            half = weighted.astype(BF16)
            rest = (both[2 * high:] - shift * (weighted - half.astype(F32))).astype(BF16)
            for field, value in enumerate((half, rest)):
                for j in range(part):
                    some = slice(LANES * j, LANES * (j + 1))
                    local[c, kind, field, j] = value[:high, some]
                    leaving[c, kind, field, j] = value[high:, some]
            field_copy(c, kind).start()

    def turn(c, source, quarter):
        first = quarter * part
        for j in range(part):
            image_wide[pl.ds(first + j, high, stride=tall)] = source[0, j].astype(F32)
            sigma[c, pl.ds(first + j, high, stride=tall)] = source[1, j].astype(F32)

    def send_image(c):
        turn(c, local.at[c, 0], group)
        turn(c, local.at[c, 1], left)
        field_copy(c, 0).wait_recv()
        turn(c, coming.at[c, 0], right)
        field_copy(c, 1).wait_recv()
        turn(c, coming.at[c, 1], opposite)

        def narrow(b, carry):
            image[c, pl.ds(b * 10, 10)] = image_wide[
                pl.ds(pl.multiple_of(b * 10 * tall, 8), 10 * tall)].astype(BF16).reshape(10, tall, LANES)
            return carry

        lax.fori_loop(0, pairs // 10, narrow, 0)

        def send(step, carry):
            forward(c, peer_at(step)).start()
            return carry

        lax.fori_loop(1, peers, send, 0)
        for j in range(spares):
            owner = stride * j + spare_place(c)

            @pl.when(owner != me)
            def _(j=j, owner=owner):
                spare_forward(c, j, owner).start()

            @pl.when(owner == me)
            def _(j=j):
                held[c, share, me] = image[c, share * peers + j]

        held[c, pl.ds(0, share), me] = image[c, pl.ds(me * share, share)]

    def apply_fock(c):
        def receive(step, carry):
            arrival(c, peer_at(step)).wait_recv()
            return carry

        lax.fori_loop(1, peers, receive, 0)
        block = jnp.concatenate([held[c, i].reshape(peers * tall, LANES) for i in range(share)], axis=1)
        product = jnp.dot(spread[...], block, preferred_element_type=F32).astype(BF16)
        for i in range(share):
            made[c, i] = product[:, LANES * i:LANES * (i + 1)].reshape(peers, tall, LANES)

        def send(step, carry):
            backward(c, peer_at(step)).start()
            return carry

        lax.fori_loop(1, peers, send, 0)
        back[c, pl.ds(me * share, share)] = made[c, pl.ds(0, share), me]

        @pl.when(owns_spare(c))
        def _():
            def receive_spare(step, carry):
                spare_arrival(c, peer_at(step)).wait_recv()
                return carry

            lax.fori_loop(1, peers, receive_spare, 0)
            one = jnp.dot(spread[...], held[c, share].reshape(peers * tall, LANES), preferred_element_type=F32)
            made[c, share] = one.astype(BF16).reshape(peers, tall, LANES)

            def send_spare(step, carry):
                spare_backward(c, peer_at(step)).start()
                return carry

            lax.fori_loop(1, peers, send_spare, 0)
            back[c, share * peers + me // stride] = made[c, share, me]

    def apply_right():
        def block(b, carry):
            own = jnp.concatenate(
                [image[c, pl.ds(b * 10, 10)].reshape(10 * tall, LANES) for c in range(chunks)], axis=1)
            product = jnp.dot(own, fock[...], preferred_element_type=F32)
            at = pl.ds(pl.multiple_of(b * 10 * tall, 8), 10 * tall)
            for c in range(chunks):
                sigma[c, at] += product[:, LANES * c:LANES * (c + 1)]
            return carry

        lax.fori_loop(0, pairs // 10, block, 0)

    def tick(n, carry):
        def stage(c, run):
            @pl.when((c >= 0) & (c < chunks))
            def _():
                run(c)

        stage(n + 1, pass_rows)
        stage(n, mix)
        stage(n + 3, send_rows)

        @pl.when(n == -2)
        def _():
            prepare()
            row_sums[0] = jnp.broadcast_to(shift_of(), (8, LANES))

        @pl.when(n == chunks + 1)
        def _():
            apply_right()

        stage(n - 2, apply_fock)
        stage(n - 1, send_image)
        return carry

    lax.fori_loop(-3, chunks + 2, tick, 0)

    shift = row_sums[0, 0:1, 0:1]
    zero = jnp.zeros((8, LANES), F32)

    def combine(c, sums):
        def receive(step, carry):
            back_arrival(c, peer_at(step)).wait_recv()
            return carry

        lax.fori_loop(1, peers, receive, 0)
        for j in range(spares):
            owner = stride * j + spare_place(c)

            @pl.when(owner != me)
            def _(j=j, owner=owner):
                spare_back_arrival(c, j, owner).wait_recv()

        def block(b, sums):
            at = pl.ds(pl.multiple_of(b * 10 * tall, 8), 10 * tall)
            some = pl.ds(b * 10, 10)
            x = trial[c, some].astype(F32).reshape(10 * tall, LANES)
            w = image[c, some].astype(F32).reshape(10 * tall, LANES)
            s = sigma[c, at] + back[c, some].astype(F32).reshape(10 * tall, LANES) - shift * w
            sigma[c, at] = s
            products = (x * s, x * w, s * s, s * w, w * w)
            return tuple(
                total + jnp.sum(term.reshape(10 * tall // 8, 8, LANES), axis=0)
                for total, term in zip(sums, products))

        return lax.fori_loop(0, pairs // 10, block, sums)

    sums = lax.fori_loop(0, chunks, combine, (zero,) * 5)
    lane = lax.broadcasted_iota(jnp.int32, (8, LANES), 1)
    packed = zero
    for q, total in enumerate(sums):
        one = jnp.sum(jnp.sum(total, axis=0, keepdims=True), axis=1, keepdims=True)
        packed = jnp.where(lane == q, one, packed)

    def sum_all(phase, value, count, place):
        row_sums[1 + phase] = value

        def copy(other, slot):
            return pltpu.make_async_remote_copy(
                src_ref=row_sums.at[1 + phase], dst_ref=sum_slots.at[phase, slot],
                send_sem=sum_sent.at[phase, other], recv_sem=sum_landed.at[phase, slot],
                device_id=place(other), device_id_type=MESH)

        mine = me if phase == 0 else group

        def send(step, carry):
            copy(lax.rem(mine + step, count), mine).start()
            return carry

        lax.fori_loop(1, count, send, 0)
        sum_slots[phase, mine] = value

        def receive(step, carry):
            other = lax.rem(mine + step, count)
            copy(other, other).wait()
            return carry

        lax.fori_loop(1, count, receive, 0)
        return jnp.sum(sum_slots[phase, pl.ds(0, count)], axis=0)

    packed = sum_all(0, packed, peers, lambda other: (group, other))
    packed = sum_all(1, packed, groups, lambda other: (other, me))
    numer, denom, ss, sw, ww = (packed[0:1, q:q + 1] for q in range(5))
    ratio = numer / denom
    norm = (ss - 2.0 * ratio * sw + ratio * ratio * ww) / denom
    stats_ref[...] = jnp.where(lane == 0, ratio + shift, norm)

    def store(c):
        return pltpu.make_async_copy(
            trial.at[c, :, real], out_ref.at[:, :, pl.ds(pl.multiple_of(c * LANES, LANES), LANES)], stored.at[c])

    def finish(c, carry):
        def block(b, carry):
            at = pl.ds(pl.multiple_of(b * 10 * tall, 8), 10 * tall)
            some = pl.ds(b * 10, 10)
            w = image[c, some].astype(F32).reshape(10 * tall, LANES)
            trial[c, some] = (sigma[c, at] - ratio * w).astype(BF16).reshape(10, tall, LANES)
            return carry

        lax.fori_loop(0, pairs // 10, block, 0)
        store(c).start()
        return carry

    lax.fori_loop(0, chunks, finish, 0)

    def drain(c, carry):
        for copy in row_sends(c) + row_forwards(c):
            copy.wait_send()
        for kind in range(2):
            field_copy(c, kind).wait_send()

        def sends(step, carry):
            forward(c, peer_at(step)).wait_send()
            backward(c, peer_at(step)).wait_send()
            return carry

        lax.fori_loop(1, peers, sends, 0)
        for j in range(spares):
            owner = stride * j + spare_place(c)

            @pl.when(owner != me)
            def _(j=j, owner=owner):
                spare_forward(c, j, owner).wait_send()

        @pl.when(owns_spare(c))
        def _():
            def spare_sends(step, carry):
                spare_backward(c, peer_at(step)).wait_send()
                return carry

            lax.fori_loop(1, peers, spare_sends, 0)

        store(c).wait()
        return carry

    lax.fori_loop(0, chunks, drain, 0)


def local(amplitudes, virtual_fock_block, metric, active_block):
    pairs, rows, width = amplitudes.shape
    peers, groups = lax.axis_size("virt"), lax.axis_size("act")
    chunks = width // LANES
    tall, high = round_up(rows, 8), round_up(pairs, 8)
    part = rows // groups
    items = pairs // peers + 1
    anywhere = pl.BlockSpec(memory_space=pl.ANY)
    dma = pltpu.SemaphoreType.DMA

    def half(*shape):
        return pltpu.VMEM(shape, BF16)

    def wide(*shape):
        return pltpu.VMEM(shape, F32)

    resid, stats = pl.pallas_call(
        functools.partial(sigma_kernel, groups, peers),
        out_shape=[
            jax.ShapeDtypeStruct(amplitudes.shape, BF16),
            jax.ShapeDtypeStruct((8, LANES), F32),
        ],
        in_specs=[anywhere] * 4,
        out_specs=[anywhere, pl.BlockSpec(memory_space=pltpu.VMEM)],
        scratch_shapes=[
            half(chunks, pairs, tall, LANES),
            half(*virtual_fock_block.shape), half(*metric.shape), half(*active_block.shape),
            half(peers * tall, peers * tall),
            half(2, groups * high, groups * high),
            half(chunks, 2, groups, part, high, LANES),
            half(chunks, 2, part, high, LANES),
            half(chunks, 2, 2, part, high, LANES),
            half(chunks, 2, 2, part, high, LANES),
            half(chunks, 2, 2, part, high, LANES),
            wide(high * tall, LANES), wide(high * tall, LANES),
            half(chunks, pairs, tall, LANES),
            half(chunks, items, peers, tall, LANES),
            half(chunks, items, peers, tall, LANES),
            half(chunks, pairs, tall, LANES),
            wide(chunks, high * tall, LANES),
            wide(3, 8, LANES),
            wide(2, peers, 8, LANES),
            dma((chunks,)), dma((3,)),
            dma((chunks, 6)), dma((chunks, 2, groups)),
            dma((chunks, 2)), dma((chunks, 2)),
            dma((chunks, peers)), dma((chunks, peers)), dma((chunks, 4)), dma((chunks, peers)),
            dma((chunks, peers)), dma((chunks, peers)), dma((chunks, peers)), dma((chunks, 4)),
            dma((chunks,)), dma((2, peers)), dma((2, peers)),
        ],
        compiler_params=pltpu.CompilerParams(
            collective_id=1, has_side_effects=True, vmem_limit_bytes=62 * 2**20),
    )(amplitudes, virtual_fock_block, metric, active_block)
    return resid, stats[0, 0], stats[0, 1]


def solution(mesh):
    return jax.shard_map(
        local,
        mesh=mesh,
        in_specs=(P("act", "virt", None), P(), P(), P()),
        out_specs=(P("act", "virt", None), P(), P()),
        check_vma=False,
    )
```

```python
import functools

import jax
import jax.numpy as jnp
from jax import lax
from jax.experimental import pallas as pl
from jax.experimental.pallas import tpu as pltpu
from jax.sharding import PartitionSpec as P

MESH = pl.DeviceIdType.MESH
LANES = 128
F32, BF16 = jnp.float32, jnp.bfloat16


def round_up(value, unit):
    return -(-value // unit) * unit


def sigma_kernel(groups, peers, x_ref, fock_ref, metric_ref, active_ref, out_ref, stats_ref,
                 own, fock, metric, active, spread, mats, gathered, fields, leaving,
                 wide, image, held, made, back, sigma, row_sums, sum_slots,
                 loaded, small_loaded, row_sent, row_landed, field_sent, field_landed, active_landed,
                 sent, landed, spare_sent, spare_landed,
                 back_sent, back_landed, back_spare_sent, back_spare_landed,
                 stored, sum_sent, sum_landed):
    group, me = lax.axis_index("act"), lax.axis_index("virt")
    chunks, pairs, tall = image.shape[0], image.shape[1], image.shape[2]
    rows, width = x_ref.shape[0], x_ref.shape[2]
    part, high = own.shape[2], own.shape[3]
    share, spares = pairs // peers, pairs % peers
    stride = peers // spares
    right, left = lax.rem(group + 1, groups), lax.rem(group + groups - 1, groups)
    opposite = lax.rem(group + 2, groups)
    others = (right, left, opposite)
    RIGHT, LEFT, OPPOSITE = range(3)
    real = pl.ds(0, rows)
    real_pairs = pl.ds(0, pairs)
    depth = 10

    def quarter(p):
        return lax.rem(group + p, groups)

    def columns(c):
        return pl.ds(pl.multiple_of(c * LANES, LANES), LANES)

    def load(c, p):
        return pltpu.make_async_copy(
            x_ref.at[pl.ds(quarter(p) * part, part), :, columns(c)], own.at[c, p, :, real_pairs], loaded.at[c])

    smalls = [pltpu.make_async_copy(source, target, small_loaded.at[i]) for i, (source, target) in enumerate(
        ((metric_ref, metric), (active_ref, active), (fock_ref, fock)))]

    def start_loads(c, carry):
        for p in range(groups):
            load(c, p).start()
        return carry

    lax.fori_loop(0, chunks, start_loads, 0)
    for copy in smalls:
        copy.start()

    barrier = pltpu.get_barrier_semaphore()
    extra = pl.ds(rows, tall - rows)
    beyond = pl.ds(pairs, high - pairs)

    def clear(c, carry):
        held[c, :, :, extra] = jnp.zeros(held.shape[1:3] + (tall - rows, LANES), BF16)
        gathered[c, :, :, :, beyond] = jnp.zeros(gathered.shape[1:4] + (high - pairs, LANES), BF16)
        own[c, :, :, beyond] = jnp.zeros(own.shape[1:3] + (high - pairs, LANES), BF16)
        fields[c, :, :, :, beyond] = jnp.zeros(fields.shape[1:4] + (high - pairs, LANES), BF16)
        return carry

    lax.fori_loop(0, chunks, clear, 0)

    def greet(step, carry):
        pl.semaphore_signal(barrier, inc=1, device_id=(group, lax.rem(me + step, peers)), device_id_type=MESH)
        return carry

    lax.fori_loop(1, peers, greet, 0)
    for step in range(1, groups):
        pl.semaphore_signal(barrier, inc=1, device_id=(lax.rem(group + step, groups), me), device_id_type=MESH)
    for q in range(tall - rows):
        wide[pl.ds(rows + q, high, stride=tall)] = jnp.zeros((high, LANES), F32)
    pl.semaphore_wait(barrier, peers + groups - 2)

    def settle(ref, semaphore):
        pltpu.make_async_copy(ref, ref, semaphore).wait()

    def row_copy(c, wave, source, kind, slot, target):
        return pltpu.make_async_remote_copy(
            src_ref=source.at[:, real_pairs], dst_ref=gathered.at[c, kind, slot, :, real_pairs],
            send_sem=row_sent.at[c], recv_sem=row_landed.at[c, wave],
            device_id=(target, me), device_id_type=MESH)

    def early_rows(c):
        return row_copy(c, 0, own.at[c, 1], 0, LEFT, right), row_copy(c, 0, own.at[c, 2], 1, RIGHT, left)

    def late_rows(c):
        return row_copy(c, 1, own.at[c, 0], 1, LEFT, right), row_copy(c, 1, own.at[c, 3], 0, RIGHT, left)

    def row_forwards(c):
        return (
            row_copy(c, 2, gathered.at[c, 0, LEFT], 1, OPPOSITE, right),
            row_copy(c, 2, gathered.at[c, 1, RIGHT], 0, OPPOSITE, left))

    def settle_rows(c, wave):
        settle(gathered.at[c, 0, pl.ds(0, 2), :, real_pairs], row_landed.at[c, wave])

    def field_copy(c, field, kind):
        return pltpu.make_async_remote_copy(
            src_ref=leaving.at[c, kind, field, :, real_pairs], dst_ref=fields.at[c, 1 + kind, field, :, real_pairs],
            send_sem=field_sent.at[c], recv_sem=active_landed.at[c] if field else field_landed.at[c, kind],
            device_id=((left, right)[kind], me), device_id_type=MESH)

    def spare_place(c):
        return lax.rem(2 * c + c // 4, stride)

    def peer_at(step):
        return lax.rem(me + step, peers)

    def forward(c, peer):
        return pltpu.make_async_remote_copy(
            src_ref=image.at[c, pl.ds(peer * share, share), real],
            dst_ref=held.at[c, pl.ds(0, share), me, real],
            send_sem=sent.at[c], recv_sem=landed.at[c],
            device_id=(group, peer), device_id_type=MESH)

    def spare_forward(c, j, peer):
        return pltpu.make_async_remote_copy(
            src_ref=image.at[c, share * peers + j, real], dst_ref=held.at[c, share, me, real],
            send_sem=spare_sent.at[c], recv_sem=spare_landed.at[c],
            device_id=(group, peer), device_id_type=MESH)

    def backward(c, peer):
        return pltpu.make_async_remote_copy(
            src_ref=made.at[c, pl.ds(0, share), peer, real],
            dst_ref=back.at[c, pl.ds(me * share, share), real],
            send_sem=back_sent.at[c], recv_sem=back_landed.at[c],
            device_id=(group, peer), device_id_type=MESH)

    def spare_backward(c, peer):
        return pltpu.make_async_remote_copy(
            src_ref=made.at[c, share, peer, real],
            dst_ref=back.at[c, share * peers + me // stride, real],
            send_sem=back_spare_sent.at[c], recv_sem=back_spare_landed.at[c],
            device_id=(group, peer), device_id_type=MESH)

    def settle_spares(c, ref, semaphore):
        mine = owns_spare(c)

        @pl.when(mine)
        def _():
            settle(ref.at[c, pl.ds(0, spares - 1), real], semaphore.at[c])

        @pl.when(jnp.logical_not(mine))
        def _():
            settle(ref.at[c, pl.ds(0, spares), real], semaphore.at[c])

    def owns_spare(c):
        return lax.rem(me, stride) == spare_place(c)

    def send_early_rows(c):
        settle(own.at[c, :, :, real_pairs], loaded.at[c])
        for copy in early_rows(c):
            copy.start()

    def send_late_rows(c):
        for copy in late_rows(c):
            copy.start()

    def prepare_mix():
        for copy in smalls:
            copy.wait()
        count = groups * pairs
        at = lax.broadcasted_iota(jnp.int32, (count, groups * high), 1)
        line = lax.broadcasted_iota(jnp.int32, (count, groups * high), 0)
        wanted = jnp.where(at - 0 * high < pairs, at + group * pairs, -1)
        for slot, other in enumerate(others):
            inside = at - (slot + 1) * high
            wanted = jnp.where(
                inside >= 0, jnp.where(inside < pairs, inside + other * pairs, -1), wanted)
        gather_pairs = jnp.where(wanted == line, 1.0, 0.0).astype(BF16)
        at = lax.broadcasted_iota(jnp.int32, (2 * high, count), 0)
        line = lax.broadcasted_iota(jnp.int32, (2 * high, count), 1)
        for which, matrix in enumerate((metric, active)):
            spaced = jnp.dot(matrix[...], gather_pairs, preferred_element_type=F32).astype(BF16)
            for kind in range(2):
                other = (left, right)[kind]
                wanted = jnp.where(at < high, at + group * pairs, at - high + other * pairs)
                kept = jnp.where(at < high, at, at - high) < pairs
                choose = jnp.where((wanted == line) & kept, 1.0, 0.0).astype(BF16)
                mats[kind, pl.ds(2 * high * which, 2 * high)] = jnp.dot(
                    choose, spaced, preferred_element_type=F32).astype(BF16)
        at = lax.broadcasted_iota(jnp.int32, fock.shape, 0)
        line = lax.broadcasted_iota(jnp.int32, fock.shape, 1)
        diagonal = jnp.where(at == line, fock[...].astype(F32), 0.0)
        trace = jnp.sum(jnp.sum(diagonal, axis=0, keepdims=True), axis=1, keepdims=True)
        row_sums[0] = jnp.broadcast_to((2.0 / width) * trace, (8, LANES))

    def prepare_spread():
        at = lax.broadcasted_iota(jnp.int32, (width, peers * tall), 0)
        line = lax.broadcasted_iota(jnp.int32, (width, peers * tall), 1)
        across = jnp.where(at + (tall - rows) * (at // rows) == line, 1.0, 0.0).astype(BF16)
        at = lax.broadcasted_iota(jnp.int32, (peers * tall, width), 1)
        line = lax.broadcasted_iota(jnp.int32, (peers * tall, width), 0)
        down = jnp.where(at + (tall - rows) * (at // rows) == line, 1.0, 0.0).astype(BF16)
        half = jnp.dot(fock[...], across, preferred_element_type=F32).astype(BF16)
        spread[...] = jnp.dot(down, half, preferred_element_type=F32).astype(BF16)

    def pass_rows(c):
        settle_rows(c, 0)
        for copy in row_forwards(c):
            copy.start()

    def mix(c):
        shift = row_sums[0, 0:1, 0:1]
        settle_rows(c, 1)
        settle_rows(c, 2)
        for kind in range(2):
            place = 3 * kind
            block = jnp.concatenate([
                jnp.concatenate(
                    [own[c, place, j]] + [gathered[c, kind, slot, j] for slot in range(groups - 1)], axis=0)
                for j in range(part)], axis=1)
            both = jnp.dot(mats[kind], block, preferred_element_type=F32)
            weighted = both[:2 * high]
            half = weighted.astype(BF16)
            rest = (both[2 * high:] - shift * (weighted - half.astype(F32))).astype(BF16)
            for field, value in enumerate((half, rest)):
                for j in range(part):
                    some = slice(LANES * j, LANES * (j + 1))
                    fields[c, place, field, j] = value[:high, some]
                    leaving[c, kind, field, j] = value[high:, some]
            field_copy(c, 0, kind).start()

    def send_active(c, carry):
        for kind in range(2):
            field_copy(c, 1, kind).start()
        return carry

    def turn(c, p):
        first = quarter(p) * part
        for j in range(part):
            wide[pl.ds(first + j, high, stride=tall)] = fields[c, p, 0, j].astype(F32)

    def send_image(c):
        turn(c, 0)
        turn(c, 3)
        field_copy(c, 0, 0).wait_recv()
        turn(c, 1)
        field_copy(c, 0, 1).wait_recv()
        turn(c, 2)

        def narrow(b, carry):
            image[c, pl.ds(b * depth, depth)] = wide[
                pl.ds(pl.multiple_of(b * depth * tall, 8), depth * tall)].astype(BF16).reshape(depth, tall, LANES)
            return carry

        lax.fori_loop(0, pairs // depth, narrow, 0)

        def send(step, carry):
            forward(c, peer_at(step)).start()
            return carry

        lax.fori_loop(1, peers, send, 0)
        for j in range(spares):
            owner = stride * j + spare_place(c)

            @pl.when(owner != me)
            def _(j=j, owner=owner):
                spare_forward(c, j, owner).start()

            @pl.when(owner == me)
            def _(j=j):
                held[c, share, me] = image[c, share * peers + j]

        held[c, pl.ds(0, share), me] = image[c, pl.ds(me * share, share)]

    def apply_fock(c):
        settle(held.at[c, pl.ds(0, share), pl.ds(0, peers - 1), real], landed.at[c])
        block = jnp.concatenate([held[c, i].reshape(peers * tall, LANES) for i in range(share)], axis=1)
        product = jnp.dot(spread[...], block, preferred_element_type=F32).astype(BF16)
        for i in range(share):
            made[c, i] = product[:, LANES * i:LANES * (i + 1)].reshape(peers, tall, LANES)

        def send(step, carry):
            backward(c, peer_at(step)).start()
            return carry

        lax.fori_loop(1, peers, send, 0)
        back[c, pl.ds(me * share, share)] = made[c, pl.ds(0, share), me]

        @pl.when(owns_spare(c))
        def _():
            settle(held.at[c, share, pl.ds(0, peers - 1), real], spare_landed.at[c])
            one = jnp.dot(spread[...], held[c, share].reshape(peers * tall, LANES), preferred_element_type=F32)
            made[c, share] = one.astype(BF16).reshape(peers, tall, LANES)

            def send_spare(step, carry):
                spare_backward(c, peer_at(step)).start()
                return carry

            lax.fori_loop(1, peers, send_spare, 0)
            back[c, share * peers + me // stride] = made[c, share, me]

    def apply_right():
        def block(p, carry):
            shift = row_sums[0, 0:1, 0:1]
            image_rows = jnp.concatenate(
                [fields[c, p, 0].reshape(part * high, LANES) for c in range(chunks)], axis=1)
            product = jnp.dot(image_rows, fock[...], preferred_element_type=F32)
            for c in range(chunks):
                sigma[c, p] = product[:, LANES * c:LANES * (c + 1)] - shift * fields[c, p, 0].reshape(
                    part * high, LANES).astype(F32)
            return carry

        lax.fori_loop(0, groups, block, 0)

    send_early_rows(0)
    send_late_rows(0)
    prepare_mix()
    pass_rows(0)
    send_early_rows(1)

    def tick(n, carry):
        def stage(c, run):
            @pl.when((c >= 0) & (c < chunks))
            def _():
                run(c)

        mix(n)
        stage(n + 1, send_late_rows)
        stage(n + 1, pass_rows)
        stage(n + 2, send_early_rows)

        @pl.when(n == 0)
        def _():
            prepare_spread()

        @pl.when(n == chunks - 2)
        def _():
            lax.fori_loop(0, 2, send_active, 0)

        @pl.when(n == chunks - 1)
        def _():
            lax.fori_loop(2, chunks, send_active, 0)

        stage(jnp.where(n < chunks - 2, n - 1, -1), apply_fock)

        send_image(n)

        @pl.when(n == chunks - 1)
        def _():
            apply_right()

        stage(jnp.where(n < chunks - 2, -1, n - 1), apply_fock)
        return carry

    lax.fori_loop(0, chunks, tick, 0)
    apply_fock(chunks - 1)

    zero = jnp.zeros((8, LANES), F32)

    def combine(c, sums):
        settle(gathered.at[c, :, :, :, real_pairs], row_sent.at[c])
        settle(own.at[c, pl.ds(0, 2), :, real_pairs], active_landed.at[c])
        settle(back.at[c, pl.ds(0, share * (peers - 1)), real], back_landed.at[c])
        settle_spares(c, back, back_spare_landed)

        def widen(b, carry):
            wide[pl.ds(pl.multiple_of(b * depth * tall, 8), depth * tall)] = back[
                c, pl.ds(b * depth, depth)].astype(F32).reshape(depth * tall, LANES)
            return carry

        lax.fori_loop(0, pairs // depth, widen, 0)

        def block(p, sums):
            first = quarter(p) * part
            for j in range(part):
                at = pl.ds(high * j, high)
                x = own[c, p, j].astype(F32)
                w = fields[c, p, 0, j].astype(F32)
                s = sigma[c, p, at] + fields[c, p, 1, j].astype(F32) + wide[pl.ds(first + j, high, stride=tall)]
                sigma[c, p, at] = s
                products = (x * s, x * w, s * s, s * w, w * w)
                sums = tuple(
                    total + jnp.sum(term.reshape(high // 8, 8, LANES), axis=0)
                    for total, term in zip(sums, products))
            return sums

        return lax.fori_loop(0, groups, block, sums)

    sums = lax.fori_loop(0, chunks, combine, (zero,) * 5)
    lane = lax.broadcasted_iota(jnp.int32, (8, LANES), 1)
    packed = zero
    for q, total in enumerate(sums):
        one = jnp.sum(jnp.sum(total, axis=0, keepdims=True), axis=1, keepdims=True)
        packed = jnp.where(lane == q, one, packed)

    def sum_all(phase, value, count, place):
        row_sums[1 + phase] = value
        mine = me if phase == 0 else group

        def copy(other, slot):
            return pltpu.make_async_remote_copy(
                src_ref=row_sums.at[1 + phase], dst_ref=sum_slots.at[phase, slot],
                send_sem=sum_sent.at[phase], recv_sem=sum_landed.at[phase],
                device_id=place(other), device_id_type=MESH)

        def send(step, carry):
            copy(lax.rem(mine + step, count), mine).start()
            return carry

        lax.fori_loop(1, count, send, 0)
        sum_slots[phase, mine] = value

        settle(sum_slots.at[phase, pl.ds(0, count - 1)], sum_landed.at[phase])
        return jnp.sum(sum_slots[phase, pl.ds(0, count)], axis=0)

    packed = sum_all(0, packed, peers, lambda other: (group, other))
    packed = sum_all(1, packed, groups, lambda other: (other, me))
    numer, denom, ss, sw, ww = (packed[0:1, q:q + 1] for q in range(5))
    ratio = numer / denom
    norm = (ss - 2.0 * ratio * sw + ratio * ratio * ww) / denom
    stats_ref[...] = jnp.where(lane == 0, ratio + row_sums[0], norm)

    def store(c, p):
        return pltpu.make_async_copy(
            own.at[c, p, :, real_pairs], out_ref.at[pl.ds(quarter(p) * part, part), :, columns(c)], stored.at[c])

    def finish(c, carry):
        def block(p, carry):
            w = fields[c, p, 0].reshape(part * high, LANES).astype(F32)
            own[c, p] = (sigma[c, p] - ratio * w).astype(BF16).reshape(part, high, LANES)
            store(c, p).start()
            return carry

        lax.fori_loop(0, groups, block, 0)
        return carry

    lax.fori_loop(0, chunks, finish, 0)

    def drain(c, carry):
        settle(leaving.at[c, :, :, :, real_pairs], field_sent.at[c])
        settle(image.at[c, pl.ds(0, share * (peers - 1)), real], sent.at[c])
        settle(made.at[c, pl.ds(0, share), pl.ds(0, peers - 1), real], back_sent.at[c])
        settle_spares(c, image, spare_sent)

        @pl.when(owns_spare(c))
        def _():
            settle(made.at[c, share, pl.ds(0, peers - 1), real], back_spare_sent.at[c])

        settle(own.at[c, :, :, real_pairs], stored.at[c])
        return carry

    lax.fori_loop(0, chunks, drain, 0)
    for phase, count in enumerate((peers, groups)):
        settle(sum_slots.at[phase, pl.ds(0, count - 1)], sum_sent.at[phase])


def local(amplitudes, virtual_fock_block, metric, active_block):
    pairs, rows, width = amplitudes.shape
    peers, groups = lax.axis_size("virt"), lax.axis_size("act")
    chunks = width // LANES
    tall, high = round_up(rows, 8), round_up(pairs, 8)
    part = rows // groups
    items = pairs // peers + 1
    anywhere = pl.BlockSpec(memory_space=pl.ANY)
    dma = pltpu.SemaphoreType.DMA

    def half(*shape):
        return pltpu.VMEM(shape, BF16)

    def full(*shape):
        return pltpu.VMEM(shape, F32)

    resid, stats = pl.pallas_call(
        functools.partial(sigma_kernel, groups, peers),
        out_shape=[
            jax.ShapeDtypeStruct((rows, pairs, width), BF16),
            jax.ShapeDtypeStruct((8, LANES), F32),
        ],
        in_specs=[anywhere] * 4,
        out_specs=[anywhere, pl.BlockSpec(memory_space=pltpu.VMEM)],
        scratch_shapes=[
            half(chunks, groups, part, high, LANES),
            half(*virtual_fock_block.shape), half(*metric.shape), half(*active_block.shape),
            half(peers * tall, peers * tall),
            half(2, groups * high, groups * high),
            half(chunks, 2, groups - 1, part, high, LANES),
            half(chunks, groups, 2, part, high, LANES),
            half(chunks, 2, 2, part, high, LANES),
            full(high * tall, LANES),
            half(chunks, pairs, tall, LANES),
            half(chunks, items, peers, tall, LANES),
            half(chunks, items, peers, tall, LANES),
            half(chunks, pairs, tall, LANES),
            full(chunks, groups, part * high, LANES),
            full(3, 8, LANES),
            full(2, peers, 8, LANES),
            dma((chunks,)), dma((3,)), dma((chunks,)), dma((chunks, 3)), dma((chunks,)), dma((chunks, 2)), dma((chunks,)),
        ] + [dma((chunks,))] * 9 + [dma((2,))] * 2,
        compiler_params=pltpu.CompilerParams(
            collective_id=1, has_side_effects=True, vmem_limit_bytes=62 * 2**20),
    )(jnp.transpose(amplitudes, (1, 0, 2)), virtual_fock_block, metric, active_block)
    return jnp.transpose(resid, (1, 0, 2)), stats[0, 0], stats[0, 1]


def solution(mesh):
    return jax.shard_map(
        local,
        mesh=mesh,
        in_specs=(P("act", "virt", None), P(), P(), P()),
        out_specs=(P("act", "virt", None), P(), P()),
        check_vma=False,
    )
```

```python
import functools

import jax
import jax.numpy as jnp
from jax import lax
from jax.experimental import pallas as pl
from jax.experimental.pallas import tpu as pltpu
from jax.sharding import PartitionSpec as P

MESH = pl.DeviceIdType.MESH
LANES = 128
F32, BF16 = jnp.float32, jnp.bfloat16


def round_up(value, unit):
    return -(-value // unit) * unit


def sigma_kernel(groups, peers, x_ref, fock_ref, metric_ref, active_ref, out_ref, stats_ref,
                 own, fock, metric, active, spread, mats, gathered, fields, leaving,
                 wide, image, held, made, back, sigma, row_sums, sum_slots,
                 loaded, small_loaded, row_sent, row_landed, field_sent, field_landed, active_landed,
                 sent, landed, spare_sent, spare_landed,
                 back_sent, back_landed, back_spare_sent, back_spare_landed,
                 sum_sent, sum_landed):
    group, me = lax.axis_index("act"), lax.axis_index("virt")
    chunks, pairs, tall = image.shape[0], image.shape[1], image.shape[2]
    rows, width = x_ref.shape[0], x_ref.shape[2]
    part, high = own.shape[2], own.shape[3]
    share, spares = pairs // peers, pairs % peers
    stride = peers // spares
    right, left = lax.rem(group + 1, groups), lax.rem(group + groups - 1, groups)
    opposite = lax.rem(group + 2, groups)
    others = (right, left, opposite)
    RIGHT, LEFT, OPPOSITE = range(3)
    real = pl.ds(0, rows)
    real_pairs = pl.ds(0, pairs)
    depth = 10

    def quarter(p):
        return lax.rem(group + p, groups)

    def columns(c):
        return pl.ds(pl.multiple_of(c * LANES, LANES), LANES)

    def load(c, p):
        return pltpu.make_async_copy(
            x_ref.at[pl.ds(quarter(p) * part, part), :, columns(c)], own.at[c, p, :, real_pairs], loaded.at[c])

    smalls = [pltpu.make_async_copy(source, target, small_loaded.at[i]) for i, (source, target) in enumerate(
        ((metric_ref, metric), (active_ref, active), (fock_ref, fock)))]

    def start_loads(c, carry):
        for p in range(groups):
            load(c, p).start()
        return carry

    lax.fori_loop(0, chunks, start_loads, 0)
    for copy in smalls:
        copy.start()

    barrier = pltpu.get_barrier_semaphore()
    extra = pl.ds(rows, tall - rows)
    beyond = pl.ds(pairs, high - pairs)

    def clear(c, carry):
        held[c, :, :, extra] = jnp.zeros(held.shape[1:3] + (tall - rows, LANES), BF16)
        gathered[c, :, :, :, beyond] = jnp.zeros(gathered.shape[1:4] + (high - pairs, LANES), BF16)
        own[c, :, :, beyond] = jnp.zeros(own.shape[1:3] + (high - pairs, LANES), BF16)
        fields[c, :, :, :, beyond] = jnp.zeros(fields.shape[1:4] + (high - pairs, LANES), BF16)
        return carry

    lax.fori_loop(0, chunks, clear, 0)

    def greet(step, carry):
        pl.semaphore_signal(barrier, inc=1, device_id=(group, lax.rem(me + step, peers)), device_id_type=MESH)
        return carry

    lax.fori_loop(1, peers, greet, 0)
    for step in range(1, groups):
        pl.semaphore_signal(barrier, inc=1, device_id=(lax.rem(group + step, groups), me), device_id_type=MESH)
    for q in range(tall - rows):
        wide[pl.ds(rows + q, high, stride=tall)] = jnp.zeros((high, LANES), F32)
    pl.semaphore_wait(barrier, peers + groups - 2)

    def settle(ref, semaphore):
        pltpu.make_async_copy(ref, ref, semaphore).wait()

    def row_copy(c, wave, source, kind, slot, target):
        return pltpu.make_async_remote_copy(
            src_ref=source.at[:, real_pairs], dst_ref=gathered.at[c, kind, slot, :, real_pairs],
            send_sem=row_sent.at[c], recv_sem=row_landed.at[c, wave],
            device_id=(target, me), device_id_type=MESH)

    def early_rows(c):
        return row_copy(c, 0, own.at[c, 1], 0, LEFT, right), row_copy(c, 0, own.at[c, 2], 1, RIGHT, left)

    def late_rows(c):
        return row_copy(c, 1, own.at[c, 0], 1, LEFT, right), row_copy(c, 1, own.at[c, 3], 0, RIGHT, left)

    def row_forwards(c):
        return (
            row_copy(c, 2, gathered.at[c, 0, LEFT], 1, OPPOSITE, right),
            row_copy(c, 2, gathered.at[c, 1, RIGHT], 0, OPPOSITE, left))

    def settle_rows(c, wave):
        settle(gathered.at[c, 0, pl.ds(0, 2), :, real_pairs], row_landed.at[c, wave])

    def field_copy(c, field, kind):
        return pltpu.make_async_remote_copy(
            src_ref=leaving.at[c, kind, field, :, real_pairs], dst_ref=fields.at[c, 1 + kind, field, :, real_pairs],
            send_sem=field_sent.at[c], recv_sem=active_landed.at[c] if field else field_landed.at[c, kind],
            device_id=((left, right)[kind], me), device_id_type=MESH)

    def spare_place(c):
        return lax.rem(2 * c + c // 4, stride)

    def peer_at(step):
        return lax.rem(me + step, peers)

    def forward(c, peer):
        return pltpu.make_async_remote_copy(
            src_ref=image.at[c, pl.ds(peer * share, share), real],
            dst_ref=held.at[c, pl.ds(0, share), me, real],
            send_sem=sent.at[c], recv_sem=landed.at[c],
            device_id=(group, peer), device_id_type=MESH)

    def spare_forward(c, j, peer):
        return pltpu.make_async_remote_copy(
            src_ref=image.at[c, share * peers + j, real], dst_ref=held.at[c, share, me, real],
            send_sem=spare_sent.at[c], recv_sem=spare_landed.at[c],
            device_id=(group, peer), device_id_type=MESH)

    def backward(c, peer):
        return pltpu.make_async_remote_copy(
            src_ref=made.at[c, pl.ds(0, share), peer, real],
            dst_ref=back.at[c, pl.ds(me * share, share), real],
            send_sem=back_sent.at[c], recv_sem=back_landed.at[c],
            device_id=(group, peer), device_id_type=MESH)

    def spare_backward(c, peer):
        return pltpu.make_async_remote_copy(
            src_ref=made.at[c, share, peer, real],
            dst_ref=back.at[c, share * peers + me // stride, real],
            send_sem=back_spare_sent.at[c], recv_sem=back_spare_landed.at[c],
            device_id=(group, peer), device_id_type=MESH)

    def settle_spares(c, ref, semaphore):
        mine = owns_spare(c)

        @pl.when(mine)
        def _():
            settle(ref.at[c, pl.ds(0, spares - 1), real], semaphore.at[c])

        @pl.when(jnp.logical_not(mine))
        def _():
            settle(ref.at[c, pl.ds(0, spares), real], semaphore.at[c])

    def owns_spare(c):
        return lax.rem(me, stride) == spare_place(c)

    def send_early_rows(c):
        settle(own.at[c, :, :, real_pairs], loaded.at[c])
        for copy in early_rows(c):
            copy.start()

    def send_late_rows(c):
        for copy in late_rows(c):
            copy.start()

    def prepare_mix():
        for copy in smalls:
            copy.wait()
        count = groups * pairs
        at = lax.broadcasted_iota(jnp.int32, (count, groups * high), 1)
        line = lax.broadcasted_iota(jnp.int32, (count, groups * high), 0)
        wanted = jnp.where(at - 0 * high < pairs, at + group * pairs, -1)
        for slot, other in enumerate(others):
            inside = at - (slot + 1) * high
            wanted = jnp.where(
                inside >= 0, jnp.where(inside < pairs, inside + other * pairs, -1), wanted)
        gather_pairs = jnp.where(wanted == line, 1.0, 0.0).astype(BF16)
        at = lax.broadcasted_iota(jnp.int32, (2 * high, count), 0)
        line = lax.broadcasted_iota(jnp.int32, (2 * high, count), 1)
        for which, matrix in enumerate((metric, active)):
            spaced = jnp.dot(matrix[...], gather_pairs, preferred_element_type=F32).astype(BF16)
            for kind in range(2):
                other = (left, right)[kind]
                wanted = jnp.where(at < high, at + group * pairs, at - high + other * pairs)
                kept = jnp.where(at < high, at, at - high) < pairs
                choose = jnp.where((wanted == line) & kept, 1.0, 0.0).astype(BF16)
                mats[kind, pl.ds(2 * high * which, 2 * high)] = jnp.dot(
                    choose, spaced, preferred_element_type=F32).astype(BF16)
        at = lax.broadcasted_iota(jnp.int32, fock.shape, 0)
        line = lax.broadcasted_iota(jnp.int32, fock.shape, 1)
        diagonal = jnp.where(at == line, fock[...].astype(F32), 0.0)
        trace = jnp.sum(jnp.sum(diagonal, axis=0, keepdims=True), axis=1, keepdims=True)
        row_sums[0] = jnp.broadcast_to((2.0 / width) * trace, (8, LANES))

    def prepare_spread():
        at = lax.broadcasted_iota(jnp.int32, (width, peers * tall), 0)
        line = lax.broadcasted_iota(jnp.int32, (width, peers * tall), 1)
        across = jnp.where(at + (tall - rows) * (at // rows) == line, 1.0, 0.0).astype(BF16)
        at = lax.broadcasted_iota(jnp.int32, (peers * tall, width), 1)
        line = lax.broadcasted_iota(jnp.int32, (peers * tall, width), 0)
        down = jnp.where(at + (tall - rows) * (at // rows) == line, 1.0, 0.0).astype(BF16)
        half = jnp.dot(fock[...], across, preferred_element_type=F32).astype(BF16)
        spread[...] = jnp.dot(down, half, preferred_element_type=F32).astype(BF16)

    def pass_rows(c):
        settle_rows(c, 0)
        for copy in row_forwards(c):
            copy.start()

    def mix(c):
        shift = row_sums[0, 0:1, 0:1]
        settle_rows(c, 1)
        settle_rows(c, 2)
        for kind in range(2):
            place = 3 * kind
            block = jnp.concatenate([
                jnp.concatenate(
                    [own[c, place, j]] + [gathered[c, kind, slot, j] for slot in range(groups - 1)], axis=0)
                for j in range(part)], axis=1)
            both = jnp.dot(mats[kind], block, preferred_element_type=F32)
            weighted = both[:2 * high]
            half = weighted.astype(BF16)
            rest = (both[2 * high:] - shift * (weighted - half.astype(F32))).astype(BF16)
            for field, value in enumerate((half, rest)):
                for j in range(part):
                    some = slice(LANES * j, LANES * (j + 1))
                    fields[c, place, field, j] = value[:high, some]
                    leaving[c, kind, field, j] = value[high:, some]
            field_copy(c, 0, kind).start()

    def send_active(c, carry):
        for kind in range(2):
            field_copy(c, 1, kind).start()
        return carry

    def turn(c, p):
        first = quarter(p) * part
        for j in range(part):
            wide[pl.ds(first + j, high, stride=tall)] = fields[c, p, 0, j].astype(F32)

    def send_image(c):
        turn(c, 0)
        turn(c, 3)
        field_copy(c, 0, 0).wait_recv()
        turn(c, 1)
        field_copy(c, 0, 1).wait_recv()
        turn(c, 2)

        def narrow(b, carry):
            image[c, pl.ds(b * depth, depth)] = wide[
                pl.ds(pl.multiple_of(b * depth * tall, 8), depth * tall)].astype(BF16).reshape(depth, tall, LANES)
            return carry

        lax.fori_loop(0, pairs // depth, narrow, 0)

        def send(step, carry):
            forward(c, peer_at(step)).start()
            return carry

        lax.fori_loop(1, peers, send, 0)
        for j in range(spares):
            owner = stride * j + spare_place(c)

            @pl.when(owner != me)
            def _(j=j, owner=owner):
                spare_forward(c, j, owner).start()

            @pl.when(owner == me)
            def _(j=j):
                held[c, share, me] = image[c, share * peers + j]

        held[c, pl.ds(0, share), me] = image[c, pl.ds(me * share, share)]

    def apply_fock(c):
        settle(held.at[c, pl.ds(0, share), pl.ds(0, peers - 1), real], landed.at[c])
        block = jnp.concatenate([held[c, i].reshape(peers * tall, LANES) for i in range(share)], axis=1)
        product = jnp.dot(spread[...], block, preferred_element_type=F32).astype(BF16)
        for i in range(share):
            made[c, i] = product[:, LANES * i:LANES * (i + 1)].reshape(peers, tall, LANES)

        def send(step, carry):
            backward(c, peer_at(step)).start()
            return carry

        lax.fori_loop(1, peers, send, 0)
        back[c, pl.ds(me * share, share)] = made[c, pl.ds(0, share), me]

        @pl.when(owns_spare(c))
        def _():
            settle(held.at[c, share, pl.ds(0, peers - 1), real], spare_landed.at[c])
            one = jnp.dot(spread[...], held[c, share].reshape(peers * tall, LANES), preferred_element_type=F32)
            made[c, share] = one.astype(BF16).reshape(peers, tall, LANES)

            def send_spare(step, carry):
                spare_backward(c, peer_at(step)).start()
                return carry

            lax.fori_loop(1, peers, send_spare, 0)
            back[c, share * peers + me // stride] = made[c, share, me]

    def apply_right():
        def block(p, carry):
            shift = row_sums[0, 0:1, 0:1]
            image_rows = jnp.concatenate(
                [fields[c, p, 0].reshape(part * high, LANES) for c in range(chunks)], axis=1)
            product = jnp.dot(image_rows, fock[...], preferred_element_type=F32)
            for c in range(chunks):
                sigma[c, p] = product[:, LANES * c:LANES * (c + 1)] - shift * fields[c, p, 0].reshape(
                    part * high, LANES).astype(F32)
            return carry

        lax.fori_loop(0, groups, block, 0)

    send_early_rows(0)
    send_late_rows(0)
    prepare_mix()
    pass_rows(0)
    send_early_rows(1)

    def tick(n, carry):
        def stage(c, run):
            @pl.when((c >= 0) & (c < chunks))
            def _():
                run(c)

        def only(k, run):
            @pl.when(n == k)
            def _():
                run()

        mix(n)
        stage(n + 1, send_late_rows)
        stage(n + 1, pass_rows)
        stage(n + 2, send_early_rows)
        only(0, prepare_spread)
        stage(jnp.where(n < chunks - 3, n - 1, -1), apply_fock)
        send_image(n)

        only(chunks - 2, lambda: lax.fori_loop(0, 2, send_active, 0))
        only(chunks - 1, lambda: lax.fori_loop(2, chunks, send_active, 0))
        stage(jnp.where(n < chunks - 3, -1, n - 1), apply_fock)
        return carry

    lax.fori_loop(0, chunks, tick, 0)
    apply_right()
    apply_fock(chunks - 1)

    zero = jnp.zeros((8, LANES), F32)

    def combine(c, sums):
        settle(gathered.at[c, :, :, :, real_pairs], row_sent.at[c])
        settle(own.at[c, pl.ds(0, 2), :, real_pairs], active_landed.at[c])
        settle(back.at[c, pl.ds(0, share * (peers - 1)), real], back_landed.at[c])
        settle_spares(c, back, back_spare_landed)

        def widen(b, carry):
            wide[pl.ds(pl.multiple_of(b * depth * tall, 8), depth * tall)] = back[
                c, pl.ds(b * depth, depth)].astype(F32).reshape(depth * tall, LANES)
            return carry

        lax.fori_loop(0, pairs // depth, widen, 0)

        def block(p, sums):
            first = quarter(p) * part
            for j in range(part):
                at = pl.ds(high * j, high)
                x = own[c, p, j].astype(F32)
                w = fields[c, p, 0, j].astype(F32)
                s = sigma[c, p, at] + fields[c, p, 1, j].astype(F32) + wide[pl.ds(first + j, high, stride=tall)]
                sigma[c, p, at] = s
                products = (x * s, x * w, s * s, s * w, w * w)
                sums = tuple(
                    total + jnp.sum(term.reshape(high // 8, 8, LANES), axis=0)
                    for total, term in zip(sums, products))
            return sums

        return lax.fori_loop(0, groups, block, sums)

    sums = lax.fori_loop(0, chunks, combine, (zero,) * 5)
    lane = lax.broadcasted_iota(jnp.int32, (8, LANES), 1)
    packed = zero
    for q, total in enumerate(sums):
        one = jnp.sum(jnp.sum(total, axis=0, keepdims=True), axis=1, keepdims=True)
        packed = jnp.where(lane == q, one, packed)

    def sum_all(phase, value, count, place):
        row_sums[1 + phase] = value
        mine = me if phase == 0 else group

        def copy(other, slot):
            return pltpu.make_async_remote_copy(
                src_ref=row_sums.at[1 + phase], dst_ref=sum_slots.at[phase, slot],
                send_sem=sum_sent.at[phase], recv_sem=sum_landed.at[phase],
                device_id=place(other), device_id_type=MESH)

        def send(step, carry):
            copy(lax.rem(mine + step, count), mine).start()
            return carry

        lax.fori_loop(1, count, send, 0)
        sum_slots[phase, mine] = value

        settle(sum_slots.at[phase, pl.ds(0, count - 1)], sum_landed.at[phase])
        return jnp.sum(sum_slots[phase, pl.ds(0, count)], axis=0)

    packed = sum_all(0, packed, peers, lambda other: (group, other))
    packed = sum_all(1, packed, groups, lambda other: (other, me))
    numer, denom, ss, sw, ww = (packed[0:1, q:q + 1] for q in range(5))
    ratio = numer / denom
    norm = (ss - 2.0 * ratio * sw + ratio * ratio * ww) / denom
    stats_ref[...] = jnp.where(lane == 0, ratio + row_sums[0], norm)

    def finish(c, carry):
        def block(p, carry):
            w = fields[c, p, 0].reshape(part * high, LANES).astype(F32)
            resid = (sigma[c, p] - ratio * w).astype(BF16).reshape(part, high, LANES)
            out_ref[pl.ds(quarter(p) * part, part), :, columns(c)] = resid[:, :pairs]
            return carry

        lax.fori_loop(0, groups, block, 0)
        return carry

    lax.fori_loop(0, chunks, finish, 0)

    def drain(c, carry):
        settle(leaving.at[c, :, :, :, real_pairs], field_sent.at[c])
        settle(image.at[c, pl.ds(0, share * (peers - 1)), real], sent.at[c])
        settle(made.at[c, pl.ds(0, share), pl.ds(0, peers - 1), real], back_sent.at[c])
        settle_spares(c, image, spare_sent)

        @pl.when(owns_spare(c))
        def _():
            settle(made.at[c, share, pl.ds(0, peers - 1), real], back_spare_sent.at[c])

        return carry

    lax.fori_loop(0, chunks, drain, 0)
    for phase, count in enumerate((peers, groups)):
        settle(sum_slots.at[phase, pl.ds(0, count - 1)], sum_sent.at[phase])


def local(amplitudes, virtual_fock_block, metric, active_block):
    pairs, rows, width = amplitudes.shape
    peers, groups = lax.axis_size("virt"), lax.axis_size("act")
    chunks = width // LANES
    tall, high = round_up(rows, 8), round_up(pairs, 8)
    part = rows // groups
    items = pairs // peers + 1
    anywhere = pl.BlockSpec(memory_space=pl.ANY)
    dma = pltpu.SemaphoreType.DMA

    def half(*shape):
        return pltpu.VMEM(shape, BF16)

    def full(*shape):
        return pltpu.VMEM(shape, F32)

    resid, stats = pl.pallas_call(
        functools.partial(sigma_kernel, groups, peers),
        out_shape=[
            jax.ShapeDtypeStruct((rows, pairs, width), BF16),
            jax.ShapeDtypeStruct((8, LANES), F32),
        ],
        in_specs=[pl.BlockSpec(memory_space=pltpu.HBM)] * 4,
        out_specs=[pl.BlockSpec(memory_space=pltpu.VMEM)] * 2,
        scratch_shapes=[
            half(chunks, groups, part, high, LANES),
            half(*virtual_fock_block.shape), half(*metric.shape), half(*active_block.shape),
            half(peers * tall, peers * tall),
            half(2, groups * high, groups * high),
            half(chunks, 2, groups - 1, part, high, LANES),
            half(chunks, groups, 2, part, high, LANES),
            half(chunks, 2, 2, part, high, LANES),
            full(high * tall, LANES),
            half(chunks, pairs, tall, LANES),
            half(chunks, items, peers, tall, LANES),
            half(chunks, items, peers, tall, LANES),
            half(chunks, pairs, tall, LANES),
            full(chunks, groups, part * high, LANES),
            full(3, 8, LANES),
            full(2, peers, 8, LANES),
            dma((chunks,)), dma((3,)), dma((chunks,)), dma((chunks, 3)), dma((chunks,)), dma((chunks, 2)), dma((chunks,)),
        ] + [dma((chunks,))] * 8 + [dma((2,))] * 2,
        compiler_params=pltpu.CompilerParams(
            collective_id=1, has_side_effects=True, vmem_limit_bytes=48 * 2**20),
    )(*(pltpu.with_memory_space_constraint(array, pltpu.HBM) for array in (
        jnp.transpose(amplitudes, (1, 0, 2)), virtual_fock_block, metric, active_block)))
    return jnp.transpose(resid, (1, 0, 2)), stats[0, 0], stats[0, 1]


def solution(mesh):
    return jax.shard_map(
        local,
        mesh=mesh,
        in_specs=(P("act", "virt", None), P(), P(), P()),
        out_specs=(P("act", "virt", None), P(), P()),
        check_vma=False,
    )
```

```python
import functools

import jax
import jax.numpy as jnp
from jax import lax
from jax.experimental import pallas as pl
from jax.experimental.pallas import tpu as pltpu
from jax.sharding import PartitionSpec as P

MESH = pl.DeviceIdType.MESH
LANES = 128
F32, BF16 = jnp.float32, jnp.bfloat16


def round_up(value, unit):
    return -(-value // unit) * unit


def sigma_kernel(groups, peers, x_ref, fock_ref, metric_ref, active_ref, out_ref, stats_ref,
                 own, fock, metric, active, spread, mats, gathered, fields, leaving,
                 wide, image, held, made, back, sigma, row_sums, sum_slots,
                 loaded, small_loaded, row_sent, row_landed, field_sent, field_landed, active_landed,
                 sent, landed, spare_sent, spare_landed,
                 back_sent, back_landed, back_spare_sent, back_spare_landed,
                 sum_sent, sum_landed):
    group, me = lax.axis_index("act"), lax.axis_index("virt")
    chunks, pairs, tall = image.shape[0], image.shape[1], image.shape[2]
    rows, width = x_ref.shape[0], x_ref.shape[2]
    part, high = own.shape[2], own.shape[3]
    share, spares = pairs // peers, pairs % peers
    stride = peers // spares
    right, left = lax.rem(group + 1, groups), lax.rem(group + groups - 1, groups)
    opposite = lax.rem(group + 2, groups)
    others = (right, left, opposite)
    RIGHT, LEFT, OPPOSITE = range(3)
    real = pl.ds(0, rows)
    real_pairs = pl.ds(0, pairs)
    depth = 10
    last = chunks - 1

    def quarter(p):
        return lax.rem(group + p, groups)

    def columns(c):
        return pl.ds(pl.multiple_of(c * LANES, LANES), LANES)

    def load(c, p):
        return pltpu.make_async_copy(
            x_ref.at[pl.ds(quarter(p) * part, part), :, columns(c)], own.at[c, p, :, real_pairs], loaded.at[c])

    smalls = [pltpu.make_async_copy(source, target, small_loaded.at[i]) for i, (source, target) in enumerate(
        ((metric_ref, metric), (active_ref, active), (fock_ref, fock)))]

    def start_loads(c, carry):
        for p in range(groups):
            load(c, p).start()
        return carry

    lax.fori_loop(0, chunks, start_loads, 0)
    for copy in smalls:
        copy.start()

    barrier = pltpu.get_barrier_semaphore()
    extra = pl.ds(rows, tall - rows)
    beyond = pl.ds(pairs, high - pairs)

    def clear(c, carry):
        held[c, :, :, extra] = jnp.zeros(held.shape[1:3] + (tall - rows, LANES), BF16)
        fields[c, :, :, :, beyond] = jnp.zeros(fields.shape[1:4] + (high - pairs, LANES), BF16)
        return carry

    def clear_rows(c, carry):
        gathered[c, :, :, :, beyond] = jnp.zeros(gathered.shape[1:4] + (high - pairs, LANES), BF16)
        own[c, :, :, beyond] = jnp.zeros(own.shape[1:3] + (high - pairs, LANES), BF16)
        return carry

    lax.fori_loop(0, chunks, clear, 0)
    lax.fori_loop(0, chunks + 1, clear_rows, 0)
    back[last, :, extra] = jnp.zeros((pairs, tall - rows, LANES), BF16)

    def greet(step, carry):
        pl.semaphore_signal(barrier, inc=1, device_id=(group, lax.rem(me + step, peers)), device_id_type=MESH)
        return carry

    lax.fori_loop(1, peers, greet, 0)
    for step in range(1, groups):
        pl.semaphore_signal(barrier, inc=1, device_id=(lax.rem(group + step, groups), me), device_id_type=MESH)
    for q in range(tall - rows):
        wide[pl.ds(rows + q, high, stride=tall)] = jnp.zeros((high, LANES), F32)
    pl.semaphore_wait(barrier, peers + groups - 2)

    def settle(ref, semaphore):
        pltpu.make_async_copy(ref, ref, semaphore).wait()

    def row_copy(c, wave, source, kind, slot, target):
        return pltpu.make_async_remote_copy(
            src_ref=source.at[:, real_pairs], dst_ref=gathered.at[c, kind, slot, :, real_pairs],
            send_sem=row_sent.at[c], recv_sem=row_landed.at[c, wave],
            device_id=(target, me), device_id_type=MESH)

    def early_rows(c):
        return row_copy(c, 0, own.at[c, 1], 0, LEFT, right), row_copy(c, 0, own.at[c, 2], 1, RIGHT, left)

    def late_rows(c):
        return row_copy(c, 1, own.at[c, 0], 1, LEFT, right), row_copy(c, 1, own.at[c, 3], 0, RIGHT, left)

    def row_forwards(c):
        return (
            row_copy(c, 2, gathered.at[c, 0, LEFT], 1, OPPOSITE, right),
            row_copy(c, 2, gathered.at[c, 1, RIGHT], 0, OPPOSITE, left))

    def settle_rows(c, wave):
        settle(gathered.at[c, 0, pl.ds(0, 2), :, real_pairs], row_landed.at[c, wave])

    def field_copy(c, field, kind):
        return pltpu.make_async_remote_copy(
            src_ref=leaving.at[c, kind, field, :, real_pairs], dst_ref=fields.at[c, 1 + kind, field, :, real_pairs],
            send_sem=field_sent.at[c], recv_sem=active_landed.at[c] if field else field_landed.at[c, kind],
            device_id=((left, right)[kind], me), device_id_type=MESH)

    def spare_place(c):
        return lax.rem(2 * c + c // 4, stride)

    def peer_at(step):
        return lax.rem(me + step, peers)

    def forward(c, peer):
        return pltpu.make_async_remote_copy(
            src_ref=image.at[c, pl.ds(peer * share, share), real],
            dst_ref=held.at[c, pl.ds(0, share), me, real],
            send_sem=sent.at[c], recv_sem=landed.at[c],
            device_id=(group, peer), device_id_type=MESH)

    def spare_forward(c, j, peer):
        return pltpu.make_async_remote_copy(
            src_ref=image.at[c, share * peers + j, real], dst_ref=held.at[c, share, me, real],
            send_sem=spare_sent.at[c], recv_sem=spare_landed.at[c],
            device_id=(group, peer), device_id_type=MESH)

    def backward(c, peer):
        return pltpu.make_async_remote_copy(
            src_ref=made.at[c, pl.ds(0, share), peer, real],
            dst_ref=back.at[c, pl.ds(me * share, share), real],
            send_sem=back_sent.at[c], recv_sem=back_landed.at[c],
            device_id=(group, peer), device_id_type=MESH)

    def spare_backward(c, peer):
        return pltpu.make_async_remote_copy(
            src_ref=made.at[c, share, peer, real],
            dst_ref=back.at[c, share * peers + me // stride, real],
            send_sem=back_spare_sent.at[c], recv_sem=back_spare_landed.at[c],
            device_id=(group, peer), device_id_type=MESH)

    def settle_spares(c, ref, semaphore):
        mine = owns_spare(c)

        @pl.when(mine)
        def _():
            settle(ref.at[c, pl.ds(0, spares - 1), real], semaphore.at[c])

        @pl.when(jnp.logical_not(mine))
        def _():
            settle(ref.at[c, pl.ds(0, spares), real], semaphore.at[c])

    def owns_spare(c):
        return lax.rem(me, stride) == spare_place(c)

    def send_early_rows(c):
        @pl.when(c < last)
        def _():
            settle(own.at[c, :, :, real_pairs], loaded.at[c])

        for copy in early_rows(c):
            copy.start()

    def send_late_rows(c):
        for copy in late_rows(c):
            copy.start()

    def prepare_mix():
        for copy in smalls:
            copy.wait()
        count = groups * pairs
        at = lax.broadcasted_iota(jnp.int32, (count, groups * high), 1)
        line = lax.broadcasted_iota(jnp.int32, (count, groups * high), 0)
        wanted = jnp.where(at - 0 * high < pairs, at + group * pairs, -1)
        for slot, other in enumerate(others):
            inside = at - (slot + 1) * high
            wanted = jnp.where(
                inside >= 0, jnp.where(inside < pairs, inside + other * pairs, -1), wanted)
        gather_pairs = jnp.where(wanted == line, 1.0, 0.0).astype(BF16)
        at = lax.broadcasted_iota(jnp.int32, (2 * high, count), 0)
        line = lax.broadcasted_iota(jnp.int32, (2 * high, count), 1)
        for which, matrix in enumerate((metric, active)):
            spaced = jnp.dot(matrix[...], gather_pairs, preferred_element_type=F32).astype(BF16)
            for kind in range(2):
                other = (left, right)[kind]
                wanted = jnp.where(at < high, at + group * pairs, at - high + other * pairs)
                kept = jnp.where(at < high, at, at - high) < pairs
                choose = jnp.where((wanted == line) & kept, 1.0, 0.0).astype(BF16)
                mats[kind, pl.ds(2 * high * which, 2 * high)] = jnp.dot(
                    choose, spaced, preferred_element_type=F32).astype(BF16)
        at = lax.broadcasted_iota(jnp.int32, fock.shape, 0)
        line = lax.broadcasted_iota(jnp.int32, fock.shape, 1)
        diagonal = jnp.where(at == line, fock[...].astype(F32), 0.0)
        trace = jnp.sum(jnp.sum(diagonal, axis=0, keepdims=True), axis=1, keepdims=True)
        row_sums[0] = jnp.broadcast_to((2.0 / width) * trace, (8, LANES))

    def prepare_spread():
        at = lax.broadcasted_iota(jnp.int32, (width, peers * tall), 0)
        line = lax.broadcasted_iota(jnp.int32, (width, peers * tall), 1)
        across = jnp.where(at + (tall - rows) * (at // rows) == line, 1.0, 0.0).astype(BF16)
        at = lax.broadcasted_iota(jnp.int32, (peers * tall, width), 1)
        line = lax.broadcasted_iota(jnp.int32, (peers * tall, width), 0)
        down = jnp.where(at + (tall - rows) * (at // rows) == line, 1.0, 0.0).astype(BF16)
        half = jnp.dot(fock[...], across, preferred_element_type=F32).astype(BF16)
        spread[...] = jnp.dot(down, half, preferred_element_type=F32).astype(BF16)

    def pass_rows(c):
        settle_rows(c, 0)
        for copy in row_forwards(c):
            copy.start()

    def block_of(c, kind):
        return jnp.concatenate([
            jnp.concatenate(
                [own[c, 3 * kind, j]] + [gathered[c, kind, slot, j] for slot in range(groups - 1)], axis=0)
            for j in range(part)], axis=1)

    def mix(c, applied=None):
        shift = row_sums[0, 0:1, 0:1]
        settle_rows(c, 1)
        settle_rows(c, 2)
        if applied is not None:
            settle_rows(applied, 1)
            settle_rows(applied, 2)
        for kind in range(2):
            place = 3 * kind
            both = jnp.dot(mats[kind], block_of(c, kind), preferred_element_type=F32)
            weighted = both[:2 * high]
            half = weighted.astype(BF16)
            rest = both[2 * high:] - shift * (weighted - half.astype(F32))
            if applied is not None:
                rest += jnp.dot(mats[kind, :2 * high], block_of(applied, kind), preferred_element_type=F32)
            rest = rest.astype(BF16)
            for field, value in enumerate((half, rest)):
                for j in range(part):
                    some = slice(LANES * j, LANES * (j + 1))
                    fields[c, place, field, j] = value[:high, some]
                    leaving[c, kind, field, j] = value[high:, some]
            field_copy(c, 0, kind).start()

    def send_active(c, carry):
        for kind in range(2):
            field_copy(c, 1, kind).start()
        return carry

    def turn(source, p):
        first = quarter(p) * part
        for j in range(part):
            wide[pl.ds(first + j, high, stride=tall)] = source[j].astype(F32)

    def send_image(c):
        turn(fields.at[c, 0, 0], 0)
        turn(fields.at[c, 3, 0], 3)
        field_copy(c, 0, 0).wait_recv()
        turn(fields.at[c, 1, 0], 1)
        field_copy(c, 0, 1).wait_recv()
        turn(fields.at[c, 2, 0], 2)
        send_slabs(c)

    def send_trial(c):
        settle(own.at[c, :, :, real_pairs], loaded.at[c])
        for p in range(groups):
            turn(own.at[c, p], p)
        send_slabs(c)

    def send_slabs(c):
        def narrow(b, carry):
            image[c, pl.ds(b * depth, depth)] = wide[
                pl.ds(pl.multiple_of(b * depth * tall, 8), depth * tall)].astype(BF16).reshape(depth, tall, LANES)
            return carry

        lax.fori_loop(0, pairs // depth, narrow, 0)

        def send(step, carry):
            forward(c, peer_at(step)).start()
            return carry

        lax.fori_loop(1, peers, send, 0)
        for j in range(spares):
            owner = stride * j + spare_place(c)

            @pl.when(owner != me)
            def _(j=j, owner=owner):
                spare_forward(c, j, owner).start()

            @pl.when(owner == me)
            def _(j=j):
                held[c, share, me] = image[c, share * peers + j]

        held[c, pl.ds(0, share), me] = image[c, pl.ds(me * share, share)]

    def apply_fock(c):
        settle(held.at[c, pl.ds(0, share), pl.ds(0, peers - 1), real], landed.at[c])
        block = jnp.concatenate([held[c, i].reshape(peers * tall, LANES) for i in range(share)], axis=1)
        product = jnp.dot(spread[...], block, preferred_element_type=F32).astype(BF16)
        for i in range(share):
            made[c, i] = product[:, LANES * i:LANES * (i + 1)].reshape(peers, tall, LANES)

        def send(step, carry):
            backward(c, peer_at(step)).start()
            return carry

        lax.fori_loop(1, peers, send, 0)
        back[c, pl.ds(me * share, share)] = made[c, pl.ds(0, share), me]

        @pl.when(owns_spare(c))
        def _():
            settle(held.at[c, share, pl.ds(0, peers - 1), real], spare_landed.at[c])
            one = jnp.dot(spread[...], held[c, share].reshape(peers * tall, LANES), preferred_element_type=F32)
            made[c, share] = one.astype(BF16).reshape(peers, tall, LANES)

            def send_spare(step, carry):
                spare_backward(c, peer_at(step)).start()
                return carry

            lax.fori_loop(1, peers, send_spare, 0)
            back[c, share * peers + me // stride] = made[c, share, me]

    def widen_back(c):
        settle(back.at[c, pl.ds(0, share * (peers - 1)), real], back_landed.at[c])
        settle_spares(c, back, back_spare_landed)

        def widen(b, carry):
            wide[pl.ds(pl.multiple_of(b * depth * tall, 8), depth * tall)] = back[
                c, pl.ds(b * depth, depth)].astype(F32).reshape(depth * tall, LANES)
            return carry

        lax.fori_loop(0, pairs // depth, widen, 0)

    def turn_applied():
        widen_back(last)
        for p in range(groups):
            first = quarter(p) * part
            for j in range(part):
                own[chunks, p, j] = wide[pl.ds(first + j, high, stride=tall)].astype(BF16)

    def apply_right():
        def block(p, carry):
            shift = row_sums[0, 0:1, 0:1]
            image_rows = jnp.concatenate(
                [fields[c, p, 0].reshape(part * high, LANES) for c in range(chunks)], axis=1)
            product = jnp.dot(image_rows, fock[...], preferred_element_type=F32)
            for c in range(chunks):
                sigma[c, p] = product[:, LANES * c:LANES * (c + 1)] - shift * fields[c, p, 0].reshape(
                    part * high, LANES).astype(F32)
            return carry

        lax.fori_loop(0, groups, block, 0)

    send_early_rows(0)
    send_late_rows(0)
    send_trial(last)
    prepare_mix()
    pass_rows(0)
    send_early_rows(1)
    prepare_spread()
    apply_fock(last)

    def tick(n, carry):
        mix(n)
        send_late_rows(n + 1)
        pass_rows(n + 1)
        send_early_rows(n + 2)

        @pl.when(n == 1)
        def _():
            apply_fock(0)

        send_image(n)

        @pl.when(n == 1)
        def _():
            turn_applied()

        @pl.when(n > 1)
        def _():
            apply_fock(n - 1)

        return carry

    lax.fori_loop(0, last, tick, 0)
    send_late_rows(chunks)
    pass_rows(chunks)
    lax.fori_loop(0, 2, send_active, 0)
    apply_fock(last - 1)
    mix(last, chunks)
    lax.fori_loop(2, chunks, send_active, 0)
    for kind in range(2):
        field_copy(last, 0, kind).wait_recv()
    apply_right()

    zero = jnp.zeros((8, LANES), F32)

    def combine(c, sums):
        settle(own.at[c, pl.ds(0, 2), :, real_pairs], active_landed.at[c])

        @pl.when(c < last)
        def _():
            widen_back(c)

        @pl.when(c == last)
        def _():
            wide[...] = jnp.zeros(wide.shape, F32)

        def block(p, sums):
            first = quarter(p) * part
            for j in range(part):
                at = pl.ds(high * j, high)
                x = own[c, p, j].astype(F32)
                w = fields[c, p, 0, j].astype(F32)
                s = sigma[c, p, at] + fields[c, p, 1, j].astype(F32) + wide[pl.ds(first + j, high, stride=tall)]
                sigma[c, p, at] = s
                products = (x * s, x * w, s * s, s * w, w * w)
                sums = tuple(
                    total + jnp.sum(term.reshape(high // 8, 8, LANES), axis=0)
                    for total, term in zip(sums, products))
            return sums

        return lax.fori_loop(0, groups, block, sums)

    sums = lax.fori_loop(0, chunks, combine, (zero,) * 5)
    lane = lax.broadcasted_iota(jnp.int32, (8, LANES), 1)
    packed = zero
    for q, total in enumerate(sums):
        one = jnp.sum(jnp.sum(total, axis=0, keepdims=True), axis=1, keepdims=True)
        packed = jnp.where(lane == q, one, packed)

    def sum_all(phase, value, count, place):
        row_sums[1 + phase] = value
        mine = me if phase == 0 else group

        def copy(other, slot):
            return pltpu.make_async_remote_copy(
                src_ref=row_sums.at[1 + phase], dst_ref=sum_slots.at[phase, slot],
                send_sem=sum_sent.at[phase], recv_sem=sum_landed.at[phase],
                device_id=place(other), device_id_type=MESH)

        def send(step, carry):
            copy(lax.rem(mine + step, count), mine).start()
            return carry

        lax.fori_loop(1, count, send, 0)
        sum_slots[phase, mine] = value

        settle(sum_slots.at[phase, pl.ds(0, count - 1)], sum_landed.at[phase])
        return jnp.sum(sum_slots[phase, pl.ds(0, count)], axis=0)

    packed = sum_all(0, packed, peers, lambda other: (group, other))
    packed = sum_all(1, packed, groups, lambda other: (other, me))
    numer, denom, ss, sw, ww = (packed[0:1, q:q + 1] for q in range(5))
    ratio = numer / denom
    norm = (ss - 2.0 * ratio * sw + ratio * ratio * ww) / denom
    stats_ref[...] = jnp.where(lane == 0, ratio + row_sums[0], norm)

    def finish(c, carry):
        def block(p, carry):
            w = fields[c, p, 0].reshape(part * high, LANES).astype(F32)
            resid = (sigma[c, p] - ratio * w).astype(BF16).reshape(part, high, LANES)
            out_ref[pl.ds(quarter(p) * part, part), :, columns(c)] = resid[:, :pairs]
            return carry

        lax.fori_loop(0, groups, block, 0)
        return carry

    lax.fori_loop(0, chunks, finish, 0)

    def drain(c, carry):
        settle(gathered.at[c, :, :, :, real_pairs], row_sent.at[c])
        settle(leaving.at[c, :, :, :, real_pairs], field_sent.at[c])
        settle(image.at[c, pl.ds(0, share * (peers - 1)), real], sent.at[c])
        settle(made.at[c, pl.ds(0, share), pl.ds(0, peers - 1), real], back_sent.at[c])
        settle_spares(c, image, spare_sent)

        @pl.when(owns_spare(c))
        def _():
            settle(made.at[c, share, pl.ds(0, peers - 1), real], back_spare_sent.at[c])

        return carry

    lax.fori_loop(0, chunks, drain, 0)
    settle(gathered.at[chunks, :, :, :, real_pairs], row_sent.at[chunks])
    for phase, count in enumerate((peers, groups)):
        settle(sum_slots.at[phase, pl.ds(0, count - 1)], sum_sent.at[phase])


def local(amplitudes, virtual_fock_block, metric, active_block):
    pairs, rows, width = amplitudes.shape
    peers, groups = lax.axis_size("virt"), lax.axis_size("act")
    chunks = width // LANES
    tall, high = round_up(rows, 8), round_up(pairs, 8)
    part = rows // groups
    items = pairs // peers + 1
    anywhere = pl.BlockSpec(memory_space=pl.ANY)
    dma = pltpu.SemaphoreType.DMA

    def half(*shape):
        return pltpu.VMEM(shape, BF16)

    def full(*shape):
        return pltpu.VMEM(shape, F32)

    resid, stats = pl.pallas_call(
        functools.partial(sigma_kernel, groups, peers),
        out_shape=[
            jax.ShapeDtypeStruct((rows, pairs, width), BF16),
            jax.ShapeDtypeStruct((8, LANES), F32),
        ],
        in_specs=[pl.BlockSpec(memory_space=pltpu.HBM)] * 4,
        out_specs=[pl.BlockSpec(memory_space=pltpu.VMEM)] * 2,
        scratch_shapes=[
            half(chunks + 1, groups, part, high, LANES),
            half(*virtual_fock_block.shape), half(*metric.shape), half(*active_block.shape),
            half(peers * tall, peers * tall),
            half(2, groups * high, groups * high),
            half(chunks + 1, 2, groups - 1, part, high, LANES),
            half(chunks, groups, 2, part, high, LANES),
            half(chunks, 2, 2, part, high, LANES),
            full(high * tall, LANES),
            half(chunks, pairs, tall, LANES),
            half(chunks, items, peers, tall, LANES),
            half(chunks, items, peers, tall, LANES),
            half(chunks, pairs, tall, LANES),
            full(chunks, groups, part * high, LANES),
            full(3, 8, LANES),
            full(2, peers, 8, LANES),
            dma((chunks,)), dma((3,)), dma((chunks + 1,)), dma((chunks + 1, 3)), dma((chunks,)), dma((chunks, 2)), dma((chunks,)),
        ] + [dma((chunks,))] * 8 + [dma((2,))] * 2,
        compiler_params=pltpu.CompilerParams(
            collective_id=1, has_side_effects=True, vmem_limit_bytes=48 * 2**20),
    )(*(pltpu.with_memory_space_constraint(array, pltpu.HBM) for array in (
        jnp.transpose(amplitudes, (1, 0, 2)), virtual_fock_block, metric, active_block)))
    return jnp.transpose(resid, (1, 0, 2)), stats[0, 0], stats[0, 1]


def solution(mesh):
    return jax.shard_map(
        local,
        mesh=mesh,
        in_specs=(P("act", "virt", None), P(), P(), P()),
        out_specs=(P("act", "virt", None), P(), P()),
        check_vma=False,
    )
```

```python
import functools

import jax
import jax.numpy as jnp
from jax import lax
from jax.experimental import pallas as pl
from jax.experimental.pallas import tpu as pltpu
from jax.sharding import PartitionSpec as P

MESH = pl.DeviceIdType.MESH
LANES = 128
F32, BF16 = jnp.float32, jnp.bfloat16


def round_up(value, unit):
    return -(-value // unit) * unit


def sigma_kernel(groups, peers, x_ref, fock_ref, metric_ref, active_ref, out_ref, stats_ref,
                 own, fock, metric, active, spread, mats, gathered, fields, leaving,
                 wide, image, held, made, back, sigma, row_sums, sum_slots,
                 loaded, small_loaded, row_sent, row_landed, field_sent, field_landed, active_landed,
                 sent, landed, spare_sent, spare_landed,
                 back_sent, back_landed, back_spare_sent, back_spare_landed,
                 sum_sent, sum_landed):
    group, me = lax.axis_index("act"), lax.axis_index("virt")
    chunks, pairs, tall = image.shape[0], image.shape[1], image.shape[2]
    rows, width = x_ref.shape[0], x_ref.shape[2]
    part, high = own.shape[2], own.shape[3]
    share, spares = pairs // peers, pairs % peers
    stride = peers // spares
    right, left = lax.rem(group + 1, groups), lax.rem(group + groups - 1, groups)
    opposite = lax.rem(group + 2, groups)
    others = (right, left, opposite)
    RIGHT, LEFT, OPPOSITE = range(3)
    real = pl.ds(0, rows)
    real_pairs = pl.ds(0, pairs)
    depth = 10
    last = chunks - 1

    def quarter(p):
        return lax.rem(group + p, groups)

    def columns(c):
        return pl.ds(pl.multiple_of(c * LANES, LANES), LANES)

    def load(c, p):
        return pltpu.make_async_copy(
            x_ref.at[pl.ds(quarter(p) * part, part), :, columns(c)], own.at[c, p, :, real_pairs], loaded.at[c])

    smalls = [pltpu.make_async_copy(source, target, small_loaded.at[i]) for i, (source, target) in enumerate(
        ((metric_ref, metric), (active_ref, active), (fock_ref, fock)))]

    def start_loads(c, carry):
        for p in range(groups):
            load(c, p).start()
        return carry

    barrier = pltpu.get_barrier_semaphore()

    def greet(step, carry):
        pl.semaphore_signal(barrier, inc=1, device_id=(group, lax.rem(me + step, peers)), device_id_type=MESH)
        return carry

    lax.fori_loop(1, peers, greet, 0)
    for step in range(1, groups):
        pl.semaphore_signal(barrier, inc=1, device_id=(lax.rem(group + step, groups), me), device_id_type=MESH)
    lax.fori_loop(0, chunks, start_loads, 0)
    for copy in smalls:
        copy.start()

    extra = pl.ds(rows, tall - rows)
    beyond = pl.ds(pairs, high - pairs)

    def clear(c, carry):
        held[c, :, :, extra] = jnp.zeros(held.shape[1:3] + (tall - rows, LANES), BF16)
        fields[c, :, :, :, beyond] = jnp.zeros(fields.shape[1:4] + (high - pairs, LANES), BF16)
        return carry

    def clear_rows(c, carry):
        gathered[c, :, :, :, beyond] = jnp.zeros(gathered.shape[1:4] + (high - pairs, LANES), BF16)
        own[c, :, :, beyond] = jnp.zeros(own.shape[1:3] + (high - pairs, LANES), BF16)
        return carry

    lax.fori_loop(0, chunks, clear, 0)
    lax.fori_loop(0, chunks + 1, clear_rows, 0)
    back[last, :, extra] = jnp.zeros((pairs, tall - rows, LANES), BF16)

    for q in range(tall - rows):
        wide[pl.ds(rows + q, high, stride=tall)] = jnp.zeros((high, LANES), F32)
    pl.semaphore_wait(barrier, peers + groups - 2)

    def settle(ref, semaphore):
        pltpu.make_async_copy(ref, ref, semaphore).wait()

    def row_copy(c, wave, source, kind, slot, target):
        return pltpu.make_async_remote_copy(
            src_ref=source.at[:, real_pairs], dst_ref=gathered.at[c, kind, slot, :, real_pairs],
            send_sem=row_sent.at[c], recv_sem=row_landed.at[c, wave],
            device_id=(target, me), device_id_type=MESH)

    def early_rows(c):
        return row_copy(c, 0, own.at[c, 1], 0, LEFT, right), row_copy(c, 0, own.at[c, 2], 1, RIGHT, left)

    def late_rows(c):
        return row_copy(c, 1, own.at[c, 0], 1, LEFT, right), row_copy(c, 1, own.at[c, 3], 0, RIGHT, left)

    def row_forwards(c):
        return (
            row_copy(c, 2, gathered.at[c, 0, LEFT], 1, OPPOSITE, right),
            row_copy(c, 2, gathered.at[c, 1, RIGHT], 0, OPPOSITE, left))

    def settle_rows(c, wave):
        settle(gathered.at[c, 0, pl.ds(0, 2), :, real_pairs], row_landed.at[c, wave])

    def field_copy(c, field, kind):
        return pltpu.make_async_remote_copy(
            src_ref=leaving.at[c, kind, field, :, real_pairs], dst_ref=fields.at[c, 1 + kind, field, :, real_pairs],
            send_sem=field_sent.at[c], recv_sem=active_landed.at[c] if field else field_landed.at[c, kind],
            device_id=((left, right)[kind], me), device_id_type=MESH)

    def spare_place(c):
        return lax.rem(2 * c + c // 4, stride)

    def peer_at(step):
        return lax.rem(me + step, peers)

    def forward(c, peer):
        return pltpu.make_async_remote_copy(
            src_ref=image.at[c, pl.ds(peer * share, share), real],
            dst_ref=held.at[c, pl.ds(0, share), me, real],
            send_sem=sent.at[c], recv_sem=landed.at[c],
            device_id=(group, peer), device_id_type=MESH)

    def spare_forward(c, j, peer):
        return pltpu.make_async_remote_copy(
            src_ref=image.at[c, share * peers + j, real], dst_ref=held.at[c, share, me, real],
            send_sem=spare_sent.at[c], recv_sem=spare_landed.at[c],
            device_id=(group, peer), device_id_type=MESH)

    def backward(c, peer):
        return pltpu.make_async_remote_copy(
            src_ref=made.at[c, pl.ds(0, share), peer, real],
            dst_ref=back.at[c, pl.ds(me * share, share), real],
            send_sem=back_sent.at[c], recv_sem=back_landed.at[c],
            device_id=(group, peer), device_id_type=MESH)

    def spare_backward(c, peer):
        return pltpu.make_async_remote_copy(
            src_ref=made.at[c, share, peer, real],
            dst_ref=back.at[c, share * peers + me // stride, real],
            send_sem=back_spare_sent.at[c], recv_sem=back_spare_landed.at[c],
            device_id=(group, peer), device_id_type=MESH)

    def settle_spares(c, ref, semaphore):
        mine = owns_spare(c)

        @pl.when(mine)
        def _():
            settle(ref.at[c, pl.ds(0, spares - 1), real], semaphore.at[c])

        @pl.when(jnp.logical_not(mine))
        def _():
            settle(ref.at[c, pl.ds(0, spares), real], semaphore.at[c])

    def owns_spare(c):
        return lax.rem(me, stride) == spare_place(c)

    def send_early_rows(c):
        @pl.when(c < last)
        def _():
            settle(own.at[c, :, :, real_pairs], loaded.at[c])

        for copy in early_rows(c):
            copy.start()

    def send_late_rows(c):
        for copy in late_rows(c):
            copy.start()

    def prepare_mix():
        for copy in smalls:
            copy.wait()
        count = groups * pairs
        at = lax.broadcasted_iota(jnp.int32, (count, groups * high), 1)
        line = lax.broadcasted_iota(jnp.int32, (count, groups * high), 0)
        wanted = jnp.where(at - 0 * high < pairs, at + group * pairs, -1)
        for slot, other in enumerate(others):
            inside = at - (slot + 1) * high
            wanted = jnp.where(
                inside >= 0, jnp.where(inside < pairs, inside + other * pairs, -1), wanted)
        gather_pairs = jnp.where(wanted == line, 1.0, 0.0).astype(BF16)
        at = lax.broadcasted_iota(jnp.int32, (2 * high, count), 0)
        line = lax.broadcasted_iota(jnp.int32, (2 * high, count), 1)
        for which, matrix in enumerate((metric, active)):
            spaced = jnp.dot(matrix[...], gather_pairs, preferred_element_type=F32).astype(BF16)
            for kind in range(2):
                other = (left, right)[kind]
                wanted = jnp.where(at < high, at + group * pairs, at - high + other * pairs)
                kept = jnp.where(at < high, at, at - high) < pairs
                choose = jnp.where((wanted == line) & kept, 1.0, 0.0).astype(BF16)
                mats[kind, pl.ds(2 * high * which, 2 * high)] = jnp.dot(
                    choose, spaced, preferred_element_type=F32).astype(BF16)
        at = lax.broadcasted_iota(jnp.int32, fock.shape, 0)
        line = lax.broadcasted_iota(jnp.int32, fock.shape, 1)
        diagonal = jnp.where(at == line, fock[...].astype(F32), 0.0)
        trace = jnp.sum(jnp.sum(diagonal, axis=0, keepdims=True), axis=1, keepdims=True)
        row_sums[0] = jnp.broadcast_to((2.0 / width) * trace, (8, LANES))

    def prepare_spread():
        at = lax.broadcasted_iota(jnp.int32, (width, peers * tall), 0)
        line = lax.broadcasted_iota(jnp.int32, (width, peers * tall), 1)
        across = jnp.where(at + (tall - rows) * (at // rows) == line, 1.0, 0.0).astype(BF16)
        at = lax.broadcasted_iota(jnp.int32, (peers * tall, width), 1)
        line = lax.broadcasted_iota(jnp.int32, (peers * tall, width), 0)
        down = jnp.where(at + (tall - rows) * (at // rows) == line, 1.0, 0.0).astype(BF16)
        half = jnp.dot(fock[...], across, preferred_element_type=F32).astype(BF16)
        spread[...] = jnp.dot(down, half, preferred_element_type=F32).astype(BF16)

    def pass_rows(c):
        settle_rows(c, 0)
        for copy in row_forwards(c):
            copy.start()

    def block_of(c, kind):
        return jnp.concatenate([
            jnp.concatenate(
                [own[c, 3 * kind, j]] + [gathered[c, kind, slot, j] for slot in range(groups - 1)], axis=0)
            for j in range(part)], axis=1)

    def mix(c):
        shift = row_sums[0, 0:1, 0:1]
        settle_rows(c, 1)
        settle_rows(c, 2)
        for kind in range(2):
            place = 3 * kind
            both = jnp.dot(mats[kind], block_of(c, kind), preferred_element_type=F32)
            weighted = both[:2 * high]
            half = weighted.astype(BF16)
            rest = (both[2 * high:] - shift * (weighted - half.astype(F32))).astype(BF16)
            for field, value in enumerate((half, rest)):
                for j in range(part):
                    some = slice(LANES * j, LANES * (j + 1))
                    fields[c, place, field, j] = value[:high, some]
                    leaving[c, kind, field, j] = value[high:, some]
            field_copy(c, 0, kind).start()

    def mix_applied():
        shift = row_sums[0, 0:1, 0:1]
        settle_rows(chunks, 1)
        settle_rows(chunks, 2)
        for kind in range(2):
            both = jnp.dot(mats[kind], block_of(last, kind), preferred_element_type=F32)
            weighted = both[:2 * high]
            rest = both[2 * high:] - shift * (weighted - weighted.astype(BF16).astype(F32))
            rest += jnp.dot(mats[kind, :2 * high], block_of(chunks, kind), preferred_element_type=F32)
            rest = rest.astype(BF16)
            for j in range(part):
                some = slice(LANES * j, LANES * (j + 1))
                fields[last, 3 * kind, 1, j] = rest[:high, some]
                leaving[last, kind, 1, j] = rest[high:, some]
            field_copy(last, 1, kind).start()

    def send_active(c, carry):
        for kind in range(2):
            field_copy(c, 1, kind).start()
        return carry

    def turn(source, p):
        first = quarter(p) * part
        for j in range(part):
            wide[pl.ds(first + j, high, stride=tall)] = source[j].astype(F32)

    def send_image(c):
        turn(fields.at[c, 0, 0], 0)
        turn(fields.at[c, 3, 0], 3)
        field_copy(c, 0, 0).wait_recv()
        turn(fields.at[c, 1, 0], 1)
        field_copy(c, 0, 1).wait_recv()
        turn(fields.at[c, 2, 0], 2)
        send_slabs(c)

    def send_trial(c):
        settle(own.at[c, :, :, real_pairs], loaded.at[c])
        for p in range(groups):
            turn(own.at[c, p], p)
        send_slabs(c)

    def send_slabs(c):
        def narrow(b, carry):
            image[c, pl.ds(b * depth, depth)] = wide[
                pl.ds(pl.multiple_of(b * depth * tall, 8), depth * tall)].astype(BF16).reshape(depth, tall, LANES)
            return carry

        lax.fori_loop(0, pairs // depth, narrow, 0)

        def send(step, carry):
            forward(c, peer_at(step)).start()
            return carry

        lax.fori_loop(1, peers, send, 0)
        for j in range(spares):
            owner = stride * j + spare_place(c)

            @pl.when(owner != me)
            def _(j=j, owner=owner):
                spare_forward(c, j, owner).start()

            @pl.when(owner == me)
            def _(j=j):
                held[c, share, me] = image[c, share * peers + j]

        held[c, pl.ds(0, share), me] = image[c, pl.ds(me * share, share)]

    def apply_fock(c):
        settle(held.at[c, pl.ds(0, share), pl.ds(0, peers - 1), real], landed.at[c])
        block = jnp.concatenate([held[c, i].reshape(peers * tall, LANES) for i in range(share)], axis=1)
        product = jnp.dot(spread[...], block, preferred_element_type=F32).astype(BF16)
        for i in range(share):
            made[c, i] = product[:, LANES * i:LANES * (i + 1)].reshape(peers, tall, LANES)

        def send(step, carry):
            backward(c, peer_at(step)).start()
            return carry

        lax.fori_loop(1, peers, send, 0)
        back[c, pl.ds(me * share, share)] = made[c, pl.ds(0, share), me]

        @pl.when(owns_spare(c))
        def _():
            settle(held.at[c, share, pl.ds(0, peers - 1), real], spare_landed.at[c])
            one = jnp.dot(spread[...], held[c, share].reshape(peers * tall, LANES), preferred_element_type=F32)
            made[c, share] = one.astype(BF16).reshape(peers, tall, LANES)

            def send_spare(step, carry):
                spare_backward(c, peer_at(step)).start()
                return carry

            lax.fori_loop(1, peers, send_spare, 0)
            back[c, share * peers + me // stride] = made[c, share, me]

    def widen_back(c):
        settle(back.at[c, pl.ds(0, share * (peers - 1)), real], back_landed.at[c])
        settle_spares(c, back, back_spare_landed)

        def widen(b, carry):
            wide[pl.ds(pl.multiple_of(b * depth * tall, 8), depth * tall)] = back[
                c, pl.ds(b * depth, depth)].astype(F32).reshape(depth * tall, LANES)
            return carry

        lax.fori_loop(0, pairs // depth, widen, 0)

    def turn_applied():
        widen_back(last)
        for p in range(groups):
            first = quarter(p) * part
            for j in range(part):
                own[chunks, p, j] = wide[pl.ds(first + j, high, stride=tall)].astype(BF16)

    def apply_right():
        def block(p, carry):
            shift = row_sums[0, 0:1, 0:1]
            image_rows = jnp.concatenate(
                [fields[c, p, 0].reshape(part * high, LANES) for c in range(chunks)], axis=1)
            product = jnp.dot(image_rows, fock[...], preferred_element_type=F32)
            for c in range(chunks):
                sigma[c, p] = product[:, LANES * c:LANES * (c + 1)] - shift * fields[c, p, 0].reshape(
                    part * high, LANES).astype(F32)
            return carry

        lax.fori_loop(0, groups, block, 0)

    send_early_rows(0)
    send_late_rows(0)
    send_trial(last)
    prepare_mix()
    pass_rows(0)
    send_early_rows(1)
    send_late_rows(1)
    prepare_spread()
    apply_fock(last)

    def tick(n, carry):
        mix(n)
        pass_rows(n + 1)

        @pl.when(n < last)
        def _():
            send_early_rows(n + 2)
            send_late_rows(n + 2)

        @pl.when(n == 1)
        def _():
            apply_fock(0)

        @pl.when(n < last)
        def _():
            send_image(n)

        @pl.when(n == 1)
        def _():
            turn_applied()

        @pl.when((n > 1) & (n < last))
        def _():
            apply_fock(n - 1)

        return carry

    lax.fori_loop(0, chunks, tick, 0)
    hurried = lax.rem(me, 2) == 1

    @pl.when(jnp.logical_not(hurried))
    def _():
        lax.fori_loop(0, last, send_active, 0)

    apply_fock(last - 1)

    @pl.when(hurried)
    def _():
        lax.fori_loop(0, last, send_active, 0)

    mix_applied()
    for kind in range(2):
        field_copy(last, 0, kind).wait_recv()
    apply_right()

    zero = jnp.zeros((8, LANES), F32)

    def combine(c, sums):
        settle(own.at[c, pl.ds(0, 2), :, real_pairs], active_landed.at[c])

        @pl.when(c < last)
        def _():
            widen_back(c)

        @pl.when(c == last)
        def _():
            wide[...] = jnp.zeros(wide.shape, F32)

        def block(p, sums):
            first = quarter(p) * part
            for j in range(part):
                at = pl.ds(high * j, high)
                x = own[c, p, j].astype(F32)
                w = fields[c, p, 0, j].astype(F32)
                s = sigma[c, p, at] + fields[c, p, 1, j].astype(F32) + wide[pl.ds(first + j, high, stride=tall)]
                sigma[c, p, at] = s
                products = (x * s, x * w, s * s, s * w, w * w)
                sums = tuple(
                    total + jnp.sum(term.reshape(high // 8, 8, LANES), axis=0)
                    for total, term in zip(sums, products))
            return sums

        return lax.fori_loop(0, groups, block, sums)

    sums = lax.fori_loop(0, chunks, combine, (zero,) * 5)
    lane = lax.broadcasted_iota(jnp.int32, (8, LANES), 1)
    packed = zero
    for q, total in enumerate(sums):
        one = jnp.sum(jnp.sum(total, axis=0, keepdims=True), axis=1, keepdims=True)
        packed = jnp.where(lane == q, one, packed)

    def sum_all(phase, value, count, place):
        row_sums[1 + phase] = value
        mine = me if phase == 0 else group

        def copy(other, slot):
            return pltpu.make_async_remote_copy(
                src_ref=row_sums.at[1 + phase], dst_ref=sum_slots.at[phase, slot],
                send_sem=sum_sent.at[phase], recv_sem=sum_landed.at[phase],
                device_id=place(other), device_id_type=MESH)

        def send(step, carry):
            copy(lax.rem(mine + step, count), mine).start()
            return carry

        lax.fori_loop(1, count, send, 0)
        sum_slots[phase, mine] = value

        settle(sum_slots.at[phase, pl.ds(0, count - 1)], sum_landed.at[phase])
        return jnp.sum(sum_slots[phase, pl.ds(0, count)], axis=0)

    packed = sum_all(0, packed, peers, lambda other: (group, other))
    packed = sum_all(1, packed, groups, lambda other: (other, me))
    numer, denom, ss, sw, ww = (packed[0:1, q:q + 1] for q in range(5))
    ratio = numer / denom
    norm = (ss - 2.0 * ratio * sw + ratio * ratio * ww) / denom
    stats_ref[...] = jnp.where(lane == 0, ratio + row_sums[0], norm)

    def finish(c, carry):
        def block(p, carry):
            w = fields[c, p, 0].reshape(part * high, LANES).astype(F32)
            resid = (sigma[c, p] - ratio * w).astype(BF16).reshape(part, high, LANES)
            out_ref[pl.ds(quarter(p) * part, part), :, columns(c)] = resid[:, :pairs]
            return carry

        lax.fori_loop(0, groups, block, 0)
        return carry

    lax.fori_loop(0, chunks, finish, 0)

    def drain(c, carry):
        settle(gathered.at[c, :, :, :, real_pairs], row_sent.at[c])
        settle(leaving.at[c, :, :, :, real_pairs], field_sent.at[c])
        settle(image.at[c, pl.ds(0, share * (peers - 1)), real], sent.at[c])
        settle(made.at[c, pl.ds(0, share), pl.ds(0, peers - 1), real], back_sent.at[c])
        settle_spares(c, image, spare_sent)

        @pl.when(owns_spare(c))
        def _():
            settle(made.at[c, share, pl.ds(0, peers - 1), real], back_spare_sent.at[c])

        return carry

    lax.fori_loop(0, chunks, drain, 0)
    settle(gathered.at[chunks, :, :, :, real_pairs], row_sent.at[chunks])
    for phase, count in enumerate((peers, groups)):
        settle(sum_slots.at[phase, pl.ds(0, count - 1)], sum_sent.at[phase])


def local(amplitudes, virtual_fock_block, metric, active_block):
    pairs, rows, width = amplitudes.shape
    peers, groups = lax.axis_size("virt"), lax.axis_size("act")
    chunks = width // LANES
    tall, high = round_up(rows, 8), round_up(pairs, 8)
    part = rows // groups
    items = pairs // peers + 1
    anywhere = pl.BlockSpec(memory_space=pl.ANY)
    dma = pltpu.SemaphoreType.DMA

    def half(*shape):
        return pltpu.VMEM(shape, BF16)

    def full(*shape):
        return pltpu.VMEM(shape, F32)

    resid, stats = pl.pallas_call(
        functools.partial(sigma_kernel, groups, peers),
        out_shape=[
            jax.ShapeDtypeStruct((rows, pairs, width), BF16),
            jax.ShapeDtypeStruct((8, LANES), F32),
        ],
        in_specs=[pl.BlockSpec(memory_space=pltpu.HBM)] * 4,
        out_specs=[pl.BlockSpec(memory_space=pltpu.VMEM)] * 2,
        scratch_shapes=[
            half(chunks + 1, groups, part, high, LANES),
            half(*virtual_fock_block.shape), half(*metric.shape), half(*active_block.shape),
            half(peers * tall, peers * tall),
            half(2, groups * high, groups * high),
            half(chunks + 1, 2, groups - 1, part, high, LANES),
            half(chunks, groups, 2, part, high, LANES),
            half(chunks, 2, 2, part, high, LANES),
            full(high * tall, LANES),
            half(chunks, pairs, tall, LANES),
            half(chunks, items, peers, tall, LANES),
            half(chunks, items, peers, tall, LANES),
            half(chunks, pairs, tall, LANES),
            full(chunks, groups, part * high, LANES),
            full(3, 8, LANES),
            full(2, peers, 8, LANES),
            dma((chunks,)), dma((3,)), dma((chunks + 1,)), dma((chunks + 1, 3)), dma((chunks,)), dma((chunks, 2)), dma((chunks,)),
        ] + [dma((chunks,))] * 8 + [dma((2,))] * 2,
        compiler_params=pltpu.CompilerParams(
            collective_id=1, has_side_effects=True, vmem_limit_bytes=48 * 2**20),
    )(*(pltpu.with_memory_space_constraint(array, pltpu.HBM) for array in (
        jnp.transpose(amplitudes, (1, 0, 2)), virtual_fock_block, metric, active_block)))
    return jnp.transpose(resid, (1, 0, 2)), stats[0, 0], stats[0, 1]


def solution(mesh):
    return jax.shard_map(
        local,
        mesh=mesh,
        in_specs=(P("act", "virt", None), P(), P(), P()),
        out_specs=(P("act", "virt", None), P(), P()),
        check_vma=False,
    )
```

```python
import functools

import jax
import jax.numpy as jnp
from jax import lax
from jax.experimental import pallas as pl
from jax.experimental.pallas import tpu as pltpu
from jax.sharding import PartitionSpec as P

MESH = pl.DeviceIdType.MESH
LANES = 128
F32, BF16 = jnp.float32, jnp.bfloat16


def round_up(value, unit):
    return -(-value // unit) * unit


def sigma_kernel(groups, peers, x_ref, fock_ref, metric_ref, active_ref, out_ref, stats_ref,
                 own, fock, metric, active, spread, mats, gathered, fields, leaving,
                 wide, image, held, made, back, sigma, row_sums, sum_slots,
                 loaded, small_loaded, row_sent, row_landed, field_sent, field_landed, active_landed,
                 sent, landed, spare_sent, spare_landed,
                 back_sent, back_landed, back_spare_sent, back_spare_landed,
                 sum_sent, sum_landed):
    group, me = lax.axis_index("act"), lax.axis_index("virt")
    chunks, pairs, tall = image.shape[0], image.shape[1], image.shape[2]
    rows, width = x_ref.shape[0], x_ref.shape[2]
    part, high = own.shape[2], own.shape[3]
    share, spares = pairs // peers, pairs % peers
    stride = peers // spares
    right, left = lax.rem(group + 1, groups), lax.rem(group + groups - 1, groups)
    opposite = lax.rem(group + 2, groups)
    others = (right, left, opposite)
    RIGHT, LEFT, OPPOSITE = range(3)
    real = pl.ds(0, rows)
    real_pairs = pl.ds(0, pairs)
    depth = 10
    last = chunks - 1

    def quarter(p):
        return lax.rem(group + p, groups)

    def columns(c):
        return pl.ds(pl.multiple_of(c * LANES, LANES), LANES)

    def load(c, p):
        return pltpu.make_async_copy(
            x_ref.at[pl.ds(quarter(p) * part, part), :, columns(c)], own.at[c, p, :, real_pairs], loaded.at[c])

    smalls = [pltpu.make_async_copy(source, target, small_loaded.at[i]) for i, (source, target) in enumerate(
        ((metric_ref, metric), (active_ref, active), (fock_ref, fock)))]

    def start_loads(c, carry):
        for p in range(groups):
            load(c, p).start()
        return carry

    barrier = pltpu.get_barrier_semaphore()

    def greet(step, carry):
        pl.semaphore_signal(barrier, inc=1, device_id=(group, lax.rem(me + step, peers)), device_id_type=MESH)
        return carry

    lax.fori_loop(1, peers, greet, 0)
    for step in range(1, groups):
        pl.semaphore_signal(barrier, inc=1, device_id=(lax.rem(group + step, groups), me), device_id_type=MESH)
    lax.fori_loop(0, chunks, start_loads, 0)
    for copy in smalls:
        copy.start()

    extra = pl.ds(rows, tall - rows)
    beyond = pl.ds(pairs, high - pairs)

    def clear(c, carry):
        held[c, :, :, extra] = jnp.zeros(held.shape[1:3] + (tall - rows, LANES), BF16)
        fields[c, :, :, :, beyond] = jnp.zeros(fields.shape[1:4] + (high - pairs, LANES), BF16)
        return carry

    def clear_rows(c, carry):
        gathered[c, :, :, :, beyond] = jnp.zeros(gathered.shape[1:4] + (high - pairs, LANES), BF16)
        own[c, :, :, beyond] = jnp.zeros(own.shape[1:3] + (high - pairs, LANES), BF16)
        return carry

    lax.fori_loop(0, chunks, clear, 0)
    lax.fori_loop(0, chunks + 1, clear_rows, 0)
    back[last, :, extra] = jnp.zeros((pairs, tall - rows, LANES), BF16)

    for q in range(tall - rows):
        wide[pl.ds(rows + q, high, stride=tall)] = jnp.zeros((high, LANES), F32)
    pl.semaphore_wait(barrier, peers + groups - 2)

    def settle(ref, semaphore):
        pltpu.make_async_copy(ref, ref, semaphore).wait()

    def row_copy(c, wave, source, kind, slot, target):
        return pltpu.make_async_remote_copy(
            src_ref=source.at[:, real_pairs], dst_ref=gathered.at[c, kind, slot, :, real_pairs],
            send_sem=row_sent.at[c], recv_sem=row_landed.at[c, wave],
            device_id=(target, me), device_id_type=MESH)

    def early_rows(c):
        return row_copy(c, 0, own.at[c, 1], 0, LEFT, right), row_copy(c, 0, own.at[c, 2], 1, RIGHT, left)

    def late_rows(c):
        return row_copy(c, 1, own.at[c, 0], 1, LEFT, right), row_copy(c, 1, own.at[c, 3], 0, RIGHT, left)

    def row_forwards(c):
        return (
            row_copy(c, 2, gathered.at[c, 0, LEFT], 1, OPPOSITE, right),
            row_copy(c, 2, gathered.at[c, 1, RIGHT], 0, OPPOSITE, left))

    def settle_rows(c, wave):
        settle(gathered.at[c, 0, pl.ds(0, 2), :, real_pairs], row_landed.at[c, wave])

    def field_copy(c, field, kind):
        return pltpu.make_async_remote_copy(
            src_ref=leaving.at[c, kind, field, :, real_pairs], dst_ref=fields.at[c, 1 + kind, field, :, real_pairs],
            send_sem=field_sent.at[c], recv_sem=active_landed.at[c] if field else field_landed.at[c, kind],
            device_id=((left, right)[kind], me), device_id_type=MESH)

    def spare_place(c):
        return lax.rem(2 * c + c // 4, stride)

    def peer_at(step):
        return lax.rem(me + step, peers)

    def forward(c, peer):
        return pltpu.make_async_remote_copy(
            src_ref=image.at[c, pl.ds(peer * share, share), real],
            dst_ref=held.at[c, pl.ds(0, share), me, real],
            send_sem=sent.at[c], recv_sem=landed.at[c],
            device_id=(group, peer), device_id_type=MESH)

    def spare_forward(c, j, peer):
        return pltpu.make_async_remote_copy(
            src_ref=image.at[c, share * peers + j, real], dst_ref=held.at[c, share, me, real],
            send_sem=spare_sent.at[c], recv_sem=spare_landed.at[c],
            device_id=(group, peer), device_id_type=MESH)

    def backward(c, peer):
        return pltpu.make_async_remote_copy(
            src_ref=made.at[c, pl.ds(0, share), peer, real],
            dst_ref=back.at[c, pl.ds(me * share, share), real],
            send_sem=back_sent.at[c], recv_sem=back_landed.at[c],
            device_id=(group, peer), device_id_type=MESH)

    def spare_backward(c, peer):
        return pltpu.make_async_remote_copy(
            src_ref=made.at[c, share, peer, real],
            dst_ref=back.at[c, share * peers + me // stride, real],
            send_sem=back_spare_sent.at[c], recv_sem=back_spare_landed.at[c],
            device_id=(group, peer), device_id_type=MESH)

    def settle_spares(c, ref, semaphore):
        mine = owns_spare(c)

        @pl.when(mine)
        def _():
            settle(ref.at[c, pl.ds(0, spares - 1), real], semaphore.at[c])

        @pl.when(jnp.logical_not(mine))
        def _():
            settle(ref.at[c, pl.ds(0, spares), real], semaphore.at[c])

    def owns_spare(c):
        return lax.rem(me, stride) == spare_place(c)

    def send_early_rows(c):
        @pl.when(c < last)
        def _():
            settle(own.at[c, :, :, real_pairs], loaded.at[c])

        for copy in early_rows(c):
            copy.start()

    def send_late_rows(c):
        for copy in late_rows(c):
            copy.start()

    def prepare_mix():
        for copy in smalls:
            copy.wait()
        count = groups * pairs
        at = lax.broadcasted_iota(jnp.int32, (count, groups * high), 1)
        line = lax.broadcasted_iota(jnp.int32, (count, groups * high), 0)
        wanted = jnp.where(at - 0 * high < pairs, at + group * pairs, -1)
        for slot, other in enumerate(others):
            inside = at - (slot + 1) * high
            wanted = jnp.where(
                inside >= 0, jnp.where(inside < pairs, inside + other * pairs, -1), wanted)
        gather_pairs = jnp.where(wanted == line, 1.0, 0.0).astype(BF16)
        at = lax.broadcasted_iota(jnp.int32, (2 * high, count), 0)
        line = lax.broadcasted_iota(jnp.int32, (2 * high, count), 1)
        for which, matrix in enumerate((metric, active)):
            spaced = jnp.dot(matrix[...], gather_pairs, preferred_element_type=F32).astype(BF16)
            for kind in range(2):
                other = (left, right)[kind]
                wanted = jnp.where(at < high, at + group * pairs, at - high + other * pairs)
                kept = jnp.where(at < high, at, at - high) < pairs
                choose = jnp.where((wanted == line) & kept, 1.0, 0.0).astype(BF16)
                mats[kind, pl.ds(2 * high * which, 2 * high)] = jnp.dot(
                    choose, spaced, preferred_element_type=F32).astype(BF16)
        at = lax.broadcasted_iota(jnp.int32, fock.shape, 0)
        line = lax.broadcasted_iota(jnp.int32, fock.shape, 1)
        diagonal = jnp.where(at == line, fock[...].astype(F32), 0.0)
        trace = jnp.sum(jnp.sum(diagonal, axis=0, keepdims=True), axis=1, keepdims=True)
        row_sums[0] = jnp.broadcast_to((2.0 / width) * trace, (8, LANES))

    def prepare_spread():
        at = lax.broadcasted_iota(jnp.int32, (width, peers * tall), 0)
        line = lax.broadcasted_iota(jnp.int32, (width, peers * tall), 1)
        across = jnp.where(at + (tall - rows) * (at // rows) == line, 1.0, 0.0).astype(BF16)
        at = lax.broadcasted_iota(jnp.int32, (peers * tall, width), 1)
        line = lax.broadcasted_iota(jnp.int32, (peers * tall, width), 0)
        down = jnp.where(at + (tall - rows) * (at // rows) == line, 1.0, 0.0).astype(BF16)
        half = jnp.dot(fock[...], across, preferred_element_type=F32).astype(BF16)
        spread[...] = jnp.dot(down, half, preferred_element_type=F32).astype(BF16)

    def pass_rows(c):
        settle_rows(c, 0)
        for copy in row_forwards(c):
            copy.start()

    def block_of(c, kind):
        return jnp.concatenate([
            jnp.concatenate(
                [own[c, 3 * kind, j]] + [gathered[c, kind, slot, j] for slot in range(groups - 1)], axis=0)
            for j in range(part)], axis=1)

    def mix(c):
        shift = row_sums[0, 0:1, 0:1]
        settle_rows(c, 1)
        settle_rows(c, 2)
        for kind in range(2):
            place = 3 * kind
            both = jnp.dot(mats[kind], block_of(c, kind), preferred_element_type=F32)
            weighted = both[:2 * high]
            half = weighted.astype(BF16)
            rest = (both[2 * high:] - shift * (weighted - half.astype(F32))).astype(BF16)
            for field, value in enumerate((half, rest)):
                for j in range(part):
                    some = slice(LANES * j, LANES * (j + 1))
                    fields[c, place, field, j] = value[:high, some]
                    leaving[c, kind, field, j] = value[high:, some]
            field_copy(c, 0, kind).start()

    def mix_applied():
        shift = row_sums[0, 0:1, 0:1]
        settle_rows(chunks, 1)
        settle_rows(chunks, 2)
        for kind in range(2):
            both = jnp.dot(mats[kind], block_of(last, kind), preferred_element_type=F32)
            weighted = both[:2 * high]
            rest = both[2 * high:] - shift * (weighted - weighted.astype(BF16).astype(F32))
            rest += jnp.dot(mats[kind, :2 * high], block_of(chunks, kind), preferred_element_type=F32)
            rest = rest.astype(BF16)
            for j in range(part):
                some = slice(LANES * j, LANES * (j + 1))
                fields[last, 3 * kind, 1, j] = rest[:high, some]
                leaving[last, kind, 1, j] = rest[high:, some]
            field_copy(last, 1, kind).start()

    def send_active(c, carry):
        for kind in range(2):
            field_copy(c, 1, kind).start()
        return carry

    def turn(source, p):
        first = quarter(p) * part
        for j in range(part):
            wide[pl.ds(first + j, high, stride=tall)] = source[j].astype(F32)

    def send_image(c):
        turn(fields.at[c, 0, 0], 0)
        turn(fields.at[c, 3, 0], 3)
        field_copy(c, 0, 0).wait_recv()
        turn(fields.at[c, 1, 0], 1)
        field_copy(c, 0, 1).wait_recv()
        turn(fields.at[c, 2, 0], 2)
        send_slabs(c)

    def send_trial(c):
        settle(own.at[c, :, :, real_pairs], loaded.at[c])
        for p in range(groups):
            turn(own.at[c, p], p)
        send_slabs(c)

    def send_slabs(c):
        def narrow(b, carry):
            image[c, pl.ds(b * depth, depth)] = wide[
                pl.ds(pl.multiple_of(b * depth * tall, 8), depth * tall)].astype(BF16).reshape(depth, tall, LANES)
            return carry

        lax.fori_loop(0, pairs // depth, narrow, 0)

        def send(step, carry):
            forward(c, peer_at(step)).start()
            return carry

        lax.fori_loop(1, peers, send, 0)
        for j in range(spares):
            owner = stride * j + spare_place(c)

            @pl.when(owner != me)
            def _(j=j, owner=owner):
                spare_forward(c, j, owner).start()

            @pl.when(owner == me)
            def _(j=j):
                held[c, share, me] = image[c, share * peers + j]

        held[c, pl.ds(0, share), me] = image[c, pl.ds(me * share, share)]

    def apply_fock(c):
        settle(held.at[c, pl.ds(0, share), pl.ds(0, peers - 1), real], landed.at[c])
        block = jnp.concatenate([held[c, i].reshape(peers * tall, LANES) for i in range(share)], axis=1)
        product = jnp.dot(spread[...], block, preferred_element_type=F32).astype(BF16)
        for i in range(share):
            made[c, i] = product[:, LANES * i:LANES * (i + 1)].reshape(peers, tall, LANES)

        def send(step, carry):
            backward(c, peer_at(step)).start()
            return carry

        lax.fori_loop(1, peers, send, 0)
        back[c, pl.ds(me * share, share)] = made[c, pl.ds(0, share), me]

        @pl.when(owns_spare(c))
        def _():
            settle(held.at[c, share, pl.ds(0, peers - 1), real], spare_landed.at[c])
            one = jnp.dot(spread[...], held[c, share].reshape(peers * tall, LANES), preferred_element_type=F32)
            made[c, share] = one.astype(BF16).reshape(peers, tall, LANES)

            def send_spare(step, carry):
                spare_backward(c, peer_at(step)).start()
                return carry

            lax.fori_loop(1, peers, send_spare, 0)
            back[c, share * peers + me // stride] = made[c, share, me]

    def widen_back(c):
        settle(back.at[c, pl.ds(0, share * (peers - 1)), real], back_landed.at[c])
        settle_spares(c, back, back_spare_landed)

        def widen(b, carry):
            wide[pl.ds(pl.multiple_of(b * depth * tall, 8), depth * tall)] = back[
                c, pl.ds(b * depth, depth)].astype(F32).reshape(depth * tall, LANES)
            return carry

        lax.fori_loop(0, pairs // depth, widen, 0)

    def turn_applied():
        widen_back(last)
        for p in range(groups):
            first = quarter(p) * part
            for j in range(part):
                own[chunks, p, j] = wide[pl.ds(first + j, high, stride=tall)].astype(BF16)

    def apply_right():
        def block(p, carry):
            shift = row_sums[0, 0:1, 0:1]
            image_rows = jnp.concatenate(
                [fields[c, p, 0].reshape(part * high, LANES) for c in range(chunks)], axis=1)
            product = jnp.dot(image_rows, fock[...], preferred_element_type=F32)
            for c in range(chunks):
                sigma[c, p] = product[:, LANES * c:LANES * (c + 1)] - shift * fields[c, p, 0].reshape(
                    part * high, LANES).astype(F32)
            return carry

        lax.fori_loop(0, groups, block, 0)

    send_early_rows(0)
    send_late_rows(0)
    send_trial(last)
    prepare_mix()
    pass_rows(0)
    send_early_rows(1)
    send_late_rows(1)
    prepare_spread()
    apply_fock(last)

    def tick(n, carry):
        mix(n)
        pass_rows(n + 1)

        @pl.when(n < last)
        def _():
            send_early_rows(n + 2)
            send_late_rows(n + 2)

        @pl.when((n == 1) | (n > 2))
        def _():
            apply_fock(jnp.where(n == 1, 0, n - 2))

        @pl.when(n < last)
        def _():
            send_image(n)

        @pl.when(n == 1)
        def _():
            turn_applied()

        return carry

    lax.fori_loop(0, chunks, tick, 0)
    hurried = lax.rem(me, 2) == 1

    @pl.when(jnp.logical_not(hurried))
    def _():
        lax.fori_loop(0, last, send_active, 0)

    apply_fock(last - 1)

    @pl.when(hurried)
    def _():
        lax.fori_loop(0, last, send_active, 0)

    mix_applied()
    for kind in range(2):
        field_copy(last, 0, kind).wait_recv()
    apply_right()

    zero = jnp.zeros((8, LANES), F32)

    def combine(c, sums):
        settle(own.at[c, pl.ds(0, 2), :, real_pairs], active_landed.at[c])

        @pl.when(c < last)
        def _():
            widen_back(c)

        @pl.when(c == last)
        def _():
            wide[...] = jnp.zeros(wide.shape, F32)

        def block(p, sums):
            first = quarter(p) * part
            for j in range(part):
                at = pl.ds(high * j, high)
                x = own[c, p, j].astype(F32)
                w = fields[c, p, 0, j].astype(F32)
                s = sigma[c, p, at] + fields[c, p, 1, j].astype(F32) + wide[pl.ds(first + j, high, stride=tall)]
                sigma[c, p, at] = s
                products = (x * s, x * w, s * s, s * w, w * w)
                sums = tuple(
                    total + jnp.sum(term.reshape(high // 8, 8, LANES), axis=0)
                    for total, term in zip(sums, products))
            return sums

        return lax.fori_loop(0, groups, block, sums)

    sums = lax.fori_loop(0, chunks, combine, (zero,) * 5)
    lane = lax.broadcasted_iota(jnp.int32, (8, LANES), 1)
    packed = zero
    for q, total in enumerate(sums):
        one = jnp.sum(jnp.sum(total, axis=0, keepdims=True), axis=1, keepdims=True)
        packed = jnp.where(lane == q, one, packed)

    def sum_all(phase, value, count, place):
        row_sums[1 + phase] = value
        mine = me if phase == 0 else group

        def copy(other, slot):
            return pltpu.make_async_remote_copy(
                src_ref=row_sums.at[1 + phase], dst_ref=sum_slots.at[phase, slot],
                send_sem=sum_sent.at[phase], recv_sem=sum_landed.at[phase],
                device_id=place(other), device_id_type=MESH)

        def send(step, carry):
            copy(lax.rem(mine + step, count), mine).start()
            return carry

        lax.fori_loop(1, count, send, 0)
        sum_slots[phase, mine] = value

        settle(sum_slots.at[phase, pl.ds(0, count - 1)], sum_landed.at[phase])
        return jnp.sum(sum_slots[phase, pl.ds(0, count)], axis=0)

    packed = sum_all(0, packed, peers, lambda other: (group, other))
    packed = sum_all(1, packed, groups, lambda other: (other, me))
    numer, denom, ss, sw, ww = (packed[0:1, q:q + 1] for q in range(5))
    ratio = numer / denom
    norm = (ss - 2.0 * ratio * sw + ratio * ratio * ww) / denom
    stats_ref[...] = jnp.where(lane == 0, ratio + row_sums[0], norm)

    def finish(c, carry):
        def block(p, carry):
            w = fields[c, p, 0].reshape(part * high, LANES).astype(F32)
            resid = (sigma[c, p] - ratio * w).astype(BF16).reshape(part, high, LANES)
            out_ref[pl.ds(quarter(p) * part, part), :, columns(c)] = resid[:, :pairs]
            return carry

        lax.fori_loop(0, groups, block, 0)
        return carry

    lax.fori_loop(0, chunks, finish, 0)

    def drain(c, carry):
        settle(gathered.at[c, :, :, :, real_pairs], row_sent.at[c])
        settle(leaving.at[c, :, :, :, real_pairs], field_sent.at[c])
        settle(image.at[c, pl.ds(0, share * (peers - 1)), real], sent.at[c])
        settle(made.at[c, pl.ds(0, share), pl.ds(0, peers - 1), real], back_sent.at[c])
        settle_spares(c, image, spare_sent)

        @pl.when(owns_spare(c))
        def _():
            settle(made.at[c, share, pl.ds(0, peers - 1), real], back_spare_sent.at[c])

        return carry

    lax.fori_loop(0, chunks, drain, 0)
    settle(gathered.at[chunks, :, :, :, real_pairs], row_sent.at[chunks])
    for phase, count in enumerate((peers, groups)):
        settle(sum_slots.at[phase, pl.ds(0, count - 1)], sum_sent.at[phase])


def local(amplitudes, virtual_fock_block, metric, active_block):
    pairs, rows, width = amplitudes.shape
    peers, groups = lax.axis_size("virt"), lax.axis_size("act")
    chunks = width // LANES
    tall, high = round_up(rows, 8), round_up(pairs, 8)
    part = rows // groups
    items = pairs // peers + 1
    anywhere = pl.BlockSpec(memory_space=pl.ANY)
    dma = pltpu.SemaphoreType.DMA

    def half(*shape):
        return pltpu.VMEM(shape, BF16)

    def full(*shape):
        return pltpu.VMEM(shape, F32)

    resid, stats = pl.pallas_call(
        functools.partial(sigma_kernel, groups, peers),
        out_shape=[
            jax.ShapeDtypeStruct((rows, pairs, width), BF16),
            jax.ShapeDtypeStruct((8, LANES), F32),
        ],
        in_specs=[pl.BlockSpec(memory_space=pltpu.HBM)] * 4,
        out_specs=[pl.BlockSpec(memory_space=pltpu.VMEM)] * 2,
        scratch_shapes=[
            half(chunks + 1, groups, part, high, LANES),
            half(*virtual_fock_block.shape), half(*metric.shape), half(*active_block.shape),
            half(peers * tall, peers * tall),
            half(2, groups * high, groups * high),
            half(chunks + 1, 2, groups - 1, part, high, LANES),
            half(chunks, groups, 2, part, high, LANES),
            half(chunks, 2, 2, part, high, LANES),
            full(high * tall, LANES),
            half(chunks, pairs, tall, LANES),
            half(chunks, items, peers, tall, LANES),
            half(chunks, items, peers, tall, LANES),
            half(chunks, pairs, tall, LANES),
            full(chunks, groups, part * high, LANES),
            full(3, 8, LANES),
            full(2, peers, 8, LANES),
            dma((chunks,)), dma((3,)), dma((chunks + 1,)), dma((chunks + 1, 3)), dma((chunks,)), dma((chunks, 2)), dma((chunks,)),
        ] + [dma((chunks,))] * 8 + [dma((2,))] * 2,
        compiler_params=pltpu.CompilerParams(
            collective_id=1, has_side_effects=True, vmem_limit_bytes=48 * 2**20),
    )(*(pltpu.with_memory_space_constraint(array, pltpu.HBM) for array in (
        jnp.transpose(amplitudes, (1, 0, 2)), virtual_fock_block, metric, active_block)))
    return jnp.transpose(resid, (1, 0, 2)), stats[0, 0], stats[0, 1]


def solution(mesh):
    return jax.shard_map(
        local,
        mesh=mesh,
        in_specs=(P("act", "virt", None), P(), P(), P()),
        out_specs=(P("act", "virt", None), P(), P()),
        check_vma=False,
    )
```
